32 devices in a mesh: gz: 4 (over z), gy: 4 (over y, x), gx: 2 (over core).
Axes of the slice: x: 2, y: 2, z: 4, core: 2. Of those that a mesh axis runs over, the one named last changes fastest.
Arguments:
- fine_now: float32 [3, 16, 64, 512], P(None, 'gz', 'gy', 'gx'), may hold values from -6 to 6
- fine_prev: float32 [3, 16, 64, 512], P(None, 'gz', 'gy', 'gx'), may hold values from -6 to 6
- stiffness: float32 [9, 16, 64, 512], P(None, 'gz', 'gy', 'gx'), may hold values from 0 to 6, as said below
- metric: float32 [16, 64, 512], P('gz', 'gy', 'gx'), may hold values from 0.7 to 1.4
- density: float32 [16, 64, 512], P('gz', 'gy', 'gx'), may hold values from 1 to 2
- coarse_now: float32 [3, 32, 32, 256], P(None, 'gz', 'gy', 'gx'), may hold values from -6 to 6
- coarse_prev: float32 [3, 32, 32, 256], P(None, 'gz', 'gy', 'gx'), may hold values from -6 to 6
- coarse_stiffness: float32 [9, 32, 32, 256], P(None, 'gz', 'gy', 'gx'), may hold values from 0 to 24, as said below
- coarse_density: float32 [32, 32, 256], P('gz', 'gy', 'gx'), may hold values from 1.5 to 3
Outputs:
- fine_next: float32 [3, 16, 64, 512], P(None, 'gz', 'gy', 'gx')
- coarse_next: float32 [3, 32, 32, 256], P(None, 'gz', 'gy', 'gx')
The draws below stay inside these ranges and needn't reach their ends.
Inputs may be any that keep to these rules, and one draw needn't show every extreme that they name: `stiffness`: channels 0 to 5 lie in [2, 6] and channels 6 to 8 in [0, 0.9]. `coarse_stiffness`: channels 0 to 5 lie in [8, 24] and channels 6 to 8 in [0, 3.6].
All inputs are finite; a program needn't handle non-finite values.
Results may differ from the reference program's by a relative error of at most 0.00002.
Values sent between devices are 32-bit elements; how exact they have to be, the bound alone decides.
No kernel may reach another device: no remote copies, remote signals or barrier semaphores. Data moves between devices by JAX's collectives and lax.ppermute only.
A program may use at most 64 MiB of HBM per device.

```python
import math
import jax
import jax.numpy as jnp
from jax import lax

ITERS = 3
NX = 512
NY = 64
NZF = 16
NZC = 32


def stiff_values(key, lowest, highest, shape):
    first_key, second_key = jax.random.split(key)
    main_part = jnp.exp(jax.random.uniform(first_key, (6,) + shape, jnp.float32, jnp.log(lowest), jnp.log(highest)))
    cross_part = jax.random.uniform(second_key, (3,) + shape, jnp.float32, 0.0, 0.45 * lowest)
    return jnp.concatenate([main_part, cross_part], 0)


def draw_stiffness(key, part):
    return stiff_values(jax.random.fold_in(key, 11), 2.0, 6.0, (NZF, NY, NX))


def draw_coarse_stiffness(key, part):
    return stiff_values(jax.random.fold_in(key, 23), 8.0, 24.0, (NZC, NY // 2, NX // 2))


def levels(key, extent, cuts, least, high):
    gain = 1.0
    for axis_at, shards_of in cuts:
        heights = jax.random.uniform(jax.random.fold_in(jax.random.fold_in(key, 6), axis_at), (shards_of,), jnp.float32, least / len(cuts), high / len(cuts))
        gain = gain * jnp.repeat(jnp.exp(heights), extent[axis_at] // shards_of).reshape((-1,) + (1,) * (len(extent) - 1 - axis_at))
    return gain


def bell_draw(stream_key, shape, width, reach, cuts=(), kind=jnp.bfloat16):
    values = jax.random.normal(stream_key, shape, jnp.float32) * width
    if len(cuts) > 0:
        values = levels(stream_key, shape, cuts, -0.22, 0.18) * values
    return jnp.clip(values, min=-reach, max=reach).astype(kind)


def setup_inputs(seed: int = 0) -> dict:
    key_of = jax.random.split(jax.random.key(seed), 10)
    return {
        "fine_now": bell_draw(key_of[0], (3, NZF, NY, NX), 1.0, 6.0, ((1, 4), (2, 4), (3, 2)), jnp.float32),
        "fine_prev": bell_draw(key_of[1], (3, NZF, NY, NX), 1.0, 6.0, ((1, 4), (2, 4), (3, 2)), jnp.float32),
        "stiffness": draw_stiffness(jax.random.fold_in(key_of[9], 71), 0),
        "metric": jnp.clip(jnp.exp(math.log(1.4) - 0.6931472 * jax.random.uniform(key_of[3], (NZF, NY, NX), jnp.float32) ** levels(key_of[3], (NZF, NY, NX), ((0, 4), (1, 4), (2, 2)), -0.2, 0.2)), 0.7, 1.4),
        "density": jnp.clip(jnp.exp(math.log(2.0) - 0.6931472 * jax.random.uniform(key_of[4], (NZF, NY, NX), jnp.float32) ** levels(key_of[4], (NZF, NY, NX), ((0, 4), (1, 4), (2, 2)), -0.2, 0.2)), 1.0, 2.0),
        "coarse_now": bell_draw(key_of[5], (3, NZC, NY // 2, NX // 2), 1.0, 6.0, ((1, 4), (2, 4), (3, 2)), jnp.float32),
        "coarse_prev": bell_draw(key_of[6], (3, NZC, NY // 2, NX // 2), 1.0, 6.0, ((1, 4), (2, 4), (3, 2)), jnp.float32),
        "coarse_stiffness": draw_coarse_stiffness(jax.random.fold_in(key_of[9], 71), 0),
        "coarse_density": jnp.clip(jnp.exp(math.log(3.0) - 0.6931472 * jax.random.uniform(key_of[8], (NZC, NY // 2, NX // 2), jnp.float32) ** levels(key_of[8], (NZC, NY // 2, NX // 2), ((0, 4), (1, 4), (2, 2)), -0.2, 0.2)), 1.5, 3.0),
    }


TIME_STEP = 0.2


def along_x(volume, inverse_step):
    return (volume[..., 1:-1, 1:-1, 2:] - volume[..., 1:-1, 1:-1, :-2]) * inverse_step


def along_y(volume, inverse_step):
    return (volume[..., 1:-1, 2:, 1:-1] - volume[..., 1:-1, :-2, 1:-1]) * inverse_step


def along_z(volume, inverse_step, stretch):
    return (volume[..., 2:, 1:-1, 1:-1] - volume[..., :-2, 1:-1, 1:-1]) * inverse_step * stretch


def stresses(padded, stiffness, stretch, inverse_step):
    disp_x, disp_y, disp_z = padded[0], padded[1], padded[2]
    normal_x = along_x(disp_x, inverse_step)
    normal_y = along_y(disp_y, inverse_step)
    normal_z = along_z(disp_z, inverse_step, stretch)
    stress_xx = stiffness[0] * normal_x + stiffness[6] * normal_y + stiffness[7] * normal_z
    stress_yy = stiffness[6] * normal_x + stiffness[1] * normal_y + stiffness[8] * normal_z
    stress_zz = stiffness[7] * normal_x + stiffness[8] * normal_y + stiffness[2] * normal_z
    stress_yz = stiffness[3] * (along_z(disp_y, inverse_step, stretch) + along_y(disp_z, inverse_step))
    stress_xz = stiffness[4] * (along_z(disp_x, inverse_step, stretch) + along_x(disp_z, inverse_step))
    stress_xy = stiffness[5] * (along_y(disp_x, inverse_step) + along_x(disp_y, inverse_step))
    return jnp.stack([stress_xx, stress_yy, stress_zz, stress_yz, stress_xz, stress_xy])


def divergence(stress, stretch, inverse_step):
    total_x = along_x(stress[0], inverse_step) + along_y(stress[5], inverse_step) + along_z(stress[4], inverse_step, stretch)
    total_y = along_x(stress[5], inverse_step) + along_y(stress[1], inverse_step) + along_z(stress[3], inverse_step, stretch)
    total_z = along_x(stress[4], inverse_step) + along_y(stress[3], inverse_step) + along_z(stress[2], inverse_step, stretch)
    return jnp.stack([total_x, total_y, total_z])


def prolong_axis(padded, axis):
    length = padded.shape[axis] - 2
    centre = lax.slice_in_dim(padded, 1, length + 1, axis=axis)
    before = lax.slice_in_dim(padded, 0, length, axis=axis)
    behind = lax.slice_in_dim(padded, 2, length + 2, axis=axis)
    even_cells = 0.75 * centre + 0.25 * before
    odd_cells = 0.75 * centre + 0.25 * behind
    new_shape = list(centre.shape)
    new_shape[axis] = 2 * length
    return jnp.stack([even_cells, odd_cells], axis + 1).reshape(new_shape)


def prolong(padded):
    return prolong_axis(prolong_axis(padded, 1), 2)


def restrict(surface):
    row_pairs = surface.reshape(surface.shape[0], surface.shape[1] // 2, 2, surface.shape[2])
    summed = row_pairs[:, :, 0] + row_pairs[:, :, 1]
    col_pairs = summed.reshape(summed.shape[0], summed.shape[1], summed.shape[2] // 2, 2)
    return (col_pairs[..., 0] + col_pairs[..., 1]) * 0.25


def advance(now, prev, stiffness, stretch, density, inverse_step):
    padded = jnp.pad(now, ((0, 0), (2, 2), (2, 2), (2, 2)))
    coef_wide = jnp.pad(stiffness, ((0, 0), (1, 1), (1, 1), (1, 1)))
    stretch_wide = jnp.pad(stretch, 1)
    inside = jnp.pad(jnp.ones(now.shape[1:], now.dtype), 1)
    stress = stresses(padded, coef_wide, stretch_wide, inverse_step) * inside
    internal = divergence(stress, stretch, inverse_step)
    return (2.0 * now - prev) + (TIME_STEP * TIME_STEP) * internal / density


def reference(fine_now, fine_prev, stiffness, metric, density, coarse_now, coarse_prev, coarse_stiffness, coarse_density):
    layers = fine_now.shape[1]
    layer_index = jnp.arange(layers)
    stretch = jnp.where((layer_index < layers // 2)[:, None, None], metric, 1.0)
    fine_step = advance(fine_now, fine_prev, stiffness, stretch, density, 0.5)
    coarse_step = advance(coarse_now, coarse_prev, coarse_stiffness, jnp.ones_like(coarse_density), coarse_density, 0.25)
    fine_start = fine_step[:, -1]
    above = fine_step[:, -2]
    fine_coef = jnp.stack([stiffness[4, -1], stiffness[3, -1], stiffness[2, -1]])
    coarse_start = coarse_step[:, 0]
    below = coarse_step[:, 1]
    coarse_coef = jnp.stack([coarse_stiffness[4, 0], coarse_stiffness[3, 0], coarse_stiffness[2, 0]])
    fine_iter = fine_start
    coarse_iter = coarse_start
    for repeat in range(ITERS):
        traction = coarse_coef * (below - coarse_iter) * 0.25
        widened = jnp.pad(traction, ((0, 0), (1, 1), (1, 1)), mode="edge")
        fine_later = above + prolong(widened) / fine_coef
        coarse_iter = 0.5 * (coarse_start + restrict(fine_iter))
        fine_iter = fine_later
    fine_next = fine_step.at[:, -1].set(fine_iter)
    coarse_next = coarse_step.at[:, 0].set(coarse_iter)
    return fine_next, coarse_next
```

```python
import numpy as np
import jax
import jax.numpy as jnp
from jax import lax
from jax.sharding import PartitionSpec as P

ITERS = 3
TIME_STEP = 0.2
HALO = 2


def pair_tables(count):
    even = [(i, i + 1) for i in range(0, count - 1, 2)]
    odd = [(i, i + 1) for i in range(1, count - 1, 2)]
    both = lambda some: some + [(b, a) for a, b in some]
    return both(even), both(odd)


def swap_both(to_prev, to_next, axis):
    count = lax.axis_size(axis)
    is_even = lax.axis_index(axis) % 2 == 0
    first, second = pair_tables(count)
    got_first = lax.ppermute(jnp.where(is_even, to_next, to_prev), axis, first)
    zero = jnp.zeros_like(got_first)
    if second:
        got_second = lax.ppermute(jnp.where(is_even, to_prev, to_next), axis, second)
    else:
        got_second = zero
    return (
        jnp.where(is_even, got_second, got_first),
        jnp.where(is_even, got_first, got_second),
    )


def flat(parts):
    return jnp.concatenate([part.reshape(-1) for part in parts])


def split(buffer, shapes):
    out = []
    at = 0
    for shape in shapes:
        size = int(np.prod(shape))
        out.append(buffer[at : at + size].reshape(shape))
        at += size
    return out


def edge(cells, dim, low, width=1):
    if low:
        return lax.slice_in_dim(cells, 0, width, axis=dim)
    return lax.slice_in_dim(cells, cells.shape[dim] - width, cells.shape[dim], axis=dim)


def faces(blocks, axis, dim):
    low = [edge(b, dim, True) for b in blocks]
    high = [edge(b, dim, False) for b in blocks]
    shapes = [f.shape for f in low]
    from_prev, from_next = swap_both(flat(low), flat(high), axis)
    return list(zip(split(from_prev, shapes), split(from_next, shapes)))


def diff(cells, around, dim, inverse_step):
    wide = jnp.concatenate([around[0], cells, around[1]], axis=dim)
    length = cells.shape[dim]
    return (
        lax.slice_in_dim(wide, 2, length + 2, axis=dim) - lax.slice_in_dim(wide, 0, length, axis=dim)
    ) * inverse_step


def stresses(disp, halos, stiffness, stretch, inverse_step):
    dx = diff(disp, halos[2], 3, inverse_step)
    dy = diff(disp, halos[1], 2, inverse_step)
    dz = diff(disp, halos[0], 1, inverse_step) * stretch
    c = stiffness
    xx = c[0] * dx[0] + c[6] * dy[1] + c[7] * dz[2]
    yy = c[6] * dx[0] + c[1] * dy[1] + c[8] * dz[2]
    zz = c[7] * dx[0] + c[8] * dy[1] + c[2] * dz[2]
    yz = c[3] * (dz[1] + dy[2])
    xz = c[4] * (dz[0] + dx[2])
    xy = c[5] * (dy[0] + dx[1])
    return (jnp.stack([xx, xy, xz]), jnp.stack([xy, yy, yz]), jnp.stack([xz, yz, zz]))


def transfer_matrices(rows, halo):
    coarse = rows + 2 * halo
    fine = 2 * rows + 4 * (halo - 1)
    up = np.zeros((fine, coarse), np.float32)
    for f in range(fine):
        c = f - 2 * (halo - 1)
        up[f, c // 2 + halo] += 0.75
        up[f, c // 2 - 1 + 2 * (c % 2) + halo] += 0.25
    return up


def prolong(plane, rows, cols, halo):
    left = transfer_matrices(rows, halo)
    right = transfer_matrices(cols, halo)
    half = jnp.einsum("fy,cyx->cfx", left, plane, precision=lax.Precision.HIGHEST)
    return jnp.einsum("cfx,gx->cfg", half, right, precision=lax.Precision.HIGHEST)


def restrict(plane):
    rows, cols = plane.shape[1] // 2, plane.shape[2] // 2
    left = np.kron(np.eye(rows, dtype=np.float32), np.full((1, 2), 0.5, np.float32))
    right = np.kron(np.eye(cols, dtype=np.float32), np.full((1, 2), 0.5, np.float32))
    half = jnp.einsum("fy,cyx->cfx", left, plane, precision=lax.Precision.HIGHEST)
    return jnp.einsum("cfx,gx->cfg", half, right, precision=lax.Precision.HIGHEST)


def clamp(plane, halo):
    for axis, dim in (("gy", 1), ("gx", 2)):
        spot = lax.axis_index(axis)
        size = plane.shape[dim]
        where = lax.broadcasted_iota(jnp.int32, plane.shape, dim)
        first = lax.slice_in_dim(plane, halo, halo + 1, axis=dim)
        last = lax.slice_in_dim(plane, size - halo - 1, size - halo, axis=dim)
        plane = jnp.where((spot == 0) & (where < halo), first, plane)
        plane = jnp.where(
            (spot == lax.axis_size(axis) - 1) & (where >= size - halo), last, plane
        )
    return plane


def trim(plane, width):
    return plane[:, width : plane.shape[1] - width, width : plane.shape[2] - width]


def widen(coarse, fine):
    for axis, dim in (("gx", 2), ("gy", 1)):
        low = [edge(p, dim, True, HALO) for p in (coarse, fine)]
        high = [edge(p, dim, False, HALO) for p in (coarse, fine)]
        shapes = [f.shape for f in low]
        prev, after = swap_both(flat(low), flat(high), axis)
        prev, after = split(prev, shapes), split(after, shapes)
        coarse = jnp.concatenate([prev[0], coarse, after[0]], axis=dim)
        fine = jnp.concatenate([prev[1], fine, after[1]], axis=dim)
    return coarse, fine


def per_device(
    fine_now,
    fine_prev,
    stiffness,
    metric,
    density,
    coarse_now,
    coarse_prev,
    coarse_stiffness,
    coarse_density,
):
    plane_z = lax.axis_index("gz")
    count_z = lax.axis_size("gz")
    layers = fine_now.shape[1]
    layer_index = plane_z * layers + jnp.arange(layers)
    stretch = jnp.where((layer_index < count_z * layers // 2)[:, None, None], metric, 1.0)

    axes = (("gz", 1), ("gy", 2), ("gx", 3))
    around = [faces([fine_now, coarse_now], axis, dim) for axis, dim in axes]
    sf = stresses(fine_now, [a[0] for a in around], stiffness, stretch, 0.5)
    sc = stresses(coarse_now, [a[1] for a in around], coarse_stiffness, 1.0, 0.25)
    by_axis = (2, 1, 0)
    around = [
        faces([sf[k], sc[k]], axis, dim) for k, (axis, dim) in zip(by_axis, axes)
    ]

    def advance(now, prev, density, stress, halos, stretch, inverse_step):
        internal = (
            diff(stress[0], halos[2], 3, inverse_step)
            + diff(stress[1], halos[1], 2, inverse_step)
            + diff(stress[2], halos[0], 1, inverse_step) * stretch
        )
        return 2.0 * now - prev + TIME_STEP * TIME_STEP * internal / density

    fine_step = advance(fine_now, fine_prev, density, sf, [a[0] for a in around], stretch, 0.5)
    coarse_step = advance(
        coarse_now, coarse_prev, coarse_density, sc, [a[1] for a in around], 1.0, 0.25
    )

    rows, cols = coarse_now.shape[2], coarse_now.shape[3]
    is_top = plane_z == count_z - 1
    above = fine_step[:, -2]
    kf = jnp.stack([stiffness[4, -1], stiffness[3, -1], stiffness[2, -1]])
    start_r = restrict(fine_step[:, -1])
    kc = jnp.stack([coarse_stiffness[4, 0], coarse_stiffness[3, 0], coarse_stiffness[2, 0]])
    coarse = jnp.concatenate([coarse_step[:, 0], coarse_step[:, 1], kc], 0)
    from_top = flat([above, kf, start_r])
    from_low = flat([coarse])
    from_low = jnp.concatenate(
        [from_low, jnp.zeros((from_top.shape[0] - from_low.shape[0],), jnp.float32)]
    )
    got = lax.ppermute(
        jnp.where(is_top, from_top, from_low), "gz", [(0, count_z - 1), (count_z - 1, 0)]
    )
    top = jnp.where(is_top, from_top, got)
    low = jnp.where(is_top, got, from_low)
    above, kf, start_r = split(top, [above.shape, kf.shape, start_r.shape])
    coarse = split(low, [coarse.shape])[0]
    coarse, fine = widen(jnp.concatenate([coarse, start_r]), jnp.concatenate([above, kf]))
    start, below, kc, start_r = (coarse[3 * i : 3 * i + 3] for i in range(4))
    above, kf = fine[:3], fine[3:]
    kf = jnp.where(kf > 0, kf, 1.0)

    traction = clamp(kc * (below - start) * 0.25, HALO)
    fine_1 = above + prolong(traction, rows, cols, HALO) / kf
    coarse_2 = 0.5 * (trim(start, 1) + restrict(fine_1))
    traction = clamp(trim(kc, 1) * (trim(below, 1) - coarse_2) * 0.25, 1)
    fine_3 = trim(above, HALO) + prolong(traction, rows, cols, 1) / trim(kf, HALO)
    coarse_1 = 0.5 * (trim(start, 1) + trim(start_r, 1))
    traction = clamp(trim(kc, 1) * (trim(below, 1) - coarse_1) * 0.25, 1)
    fine_2 = trim(above, HALO) + prolong(traction, rows, cols, 1) / trim(kf, HALO)
    coarse_3 = 0.5 * (trim(start, HALO) + restrict(fine_2))

    fine_next = fine_step.at[:, -1].set(jnp.where(is_top, fine_3, fine_step[:, -1]))
    coarse_next = coarse_step.at[:, 0].set(
        jnp.where(plane_z == 0, coarse_3, coarse_step[:, 0])
    )
    return (fine_next, coarse_next)


def solution(mesh):
    block = P(None, "gz", "gy", "gx")
    field = P("gz", "gy", "gx")
    return jax.shard_map(
        per_device,
        mesh=mesh,
        in_specs=(block, block, block, field, field, block, block, block, field),
        out_specs=(block, block),
        check_vma=False,
    )
```

```python
import functools

import numpy as np
import jax
import jax.numpy as jnp
from jax import lax
from jax.experimental import pallas as pl
from jax.experimental.pallas import tpu as pltpu
from jax.sharding import PartitionSpec as P

ITERS = 3
TIME_STEP = 0.2
ALPHA = TIME_STEP * TIME_STEP
SUB = 8
LANE = 128
COLS = 4
SLOTS = LANE // COLS
Y_CHANNELS = (1, 3, 5, 6, 8)
Z_CHANNELS = (2, 3, 4, 7, 8)
XX, YY, ZZ, YZ, XZ, XY = range(6)


class Block:
    def __init__(self, shape, fine):
        self.layers, self.rows, self.cols = shape
        self.fine = fine
        self.inverse_step = 0.5 if fine else 0.25
        self.wide = (self.rows + SUB, self.cols + LANE)
        self.row_tiles, self.col_tiles = self.rows // SUB, self.cols // LANE
        self.planes = []
        for layer in range(self.layers):
            depth = self.depth(layer)
            for c in range(3):
                self.planes.append(("u", c, layer, 4 if depth < 4 else 2))
            for c in range(9):
                in_y, in_z = c in Y_CHANNELS, c in Z_CHANNELS
                if depth < 2:
                    count = 3 if in_y else 2
                elif depth == 2 and in_z:
                    count = 2
                else:
                    count = 1 if in_y else 0
                self.planes.append(("k", c, layer, count))
            if fine:
                self.planes.append(("m", 0, layer, 1))
            if depth < 2:
                for c in range(3):
                    self.planes.append(("p", c, layer, 2))
                self.planes.append(("d", 0, layer, 2))
        self.index = {plane[:3]: i for i, plane in enumerate(self.planes)}

    def depth(self, layer):
        return self.layers - 1 - layer if self.fine else layer

    def x_tiles(self):
        return -(-len(self.planes) // SLOTS) * (self.row_tiles + 1)


def row_table(blocks):
    table, at = {}, 0
    for count in (4, 2, 1, 3):
        for b, block in enumerate(blocks):
            for p, plane in enumerate(block.planes):
                if plane[3] == count:
                    for t in range(block.col_tiles):
                        table[b, p, t] = at
                        at += count
    return table, -(-at // SUB) * SUB


def lanes_of(t):
    return slice(LANE * t, LANE * t + LANE)


def rows_of(t):
    return slice(SUB * t, SUB * t + SUB)


def own(refs, plane, rows, lanes):
    kind, c, layer = plane[:3]
    if kind in ("m", "d"):
        return refs[kind][layer, rows, lanes]
    return refs[kind][c, layer, rows, lanes]


def is_even(axis):
    return lax.rem(lax.axis_index(axis), 2) == 0


def iota(shape, dim):
    return lax.broadcasted_iota(jnp.int32, shape, dim)


def named(refs):
    fine = dict(zip("ukmpd", refs[:5]))
    coarse = dict(zip("ukpd", refs[5:9]))
    return (fine, coarse), refs[9:]


def rows_kernel(blocks, *refs):
    sources, (first, second) = named(refs)
    table, _ = row_table(blocks)
    even = is_even("gy")
    for b, block in enumerate(blocks):
        for p, plane in enumerate(block.planes):
            count = plane[3]
            for t in range(block.col_tiles if count else 0):
                high = own(sources[b], plane, slice(block.rows - count, block.rows), lanes_of(t))
                low = own(sources[b], plane, slice(0, count), lanes_of(t))
                at = slice(table[b, p, t], table[b, p, t] + count)
                first[at, :] = lax.select(even, high, low)
                second[at, :] = lax.select(even, low, high)


def columns_kernel(blocks, both, *refs):
    sources, rest = named(refs)
    got_first, got_second = rest[:2]
    halos = rest[2:4]
    outs = rest[4:]
    table, _ = row_table(blocks)
    even = is_even("gy")
    for b, block in enumerate(blocks):
        for p, plane in enumerate(block.planes):
            count = plane[3]
            halos[b][p] = jnp.zeros((SUB, block.cols), jnp.float32)
            for t in range(block.col_tiles if count else 0):
                at = slice(table[b, p, t], table[b, p, t] + count)
                one, two = got_first[at, :], got_second[at, :]
                halos[b][p, 0:count, lanes_of(t)] = lax.select(even, one, two)
                halos[b][p, SUB - count : SUB, lanes_of(t)] = lax.select(even, two, one)
    even = is_even("gx")
    lane = iota((SUB, LANE), 1)
    slot = lax.shift_right_logical(lane, jnp.full((SUB, LANE), 2, jnp.int32))
    move = lax.select(even, jnp.int32(COLS), jnp.int32(0))
    back = COLS - move
    at = 0
    for b, block in enumerate(blocks):
        for group in range(0, len(block.planes), SLOTS):
            for rt in range(block.row_tiles + 1):
                made = [jnp.zeros((SUB, LANE), jnp.float32) for _ in outs]
                for s, plane in enumerate(block.planes[group : group + SLOTS]):
                    if rt < block.row_tiles:
                        left = own(sources[b], plane, rows_of(rt), lanes_of(0))
                        right = own(sources[b], plane, rows_of(rt), lanes_of(block.col_tiles - 1))
                    elif plane[3]:
                        left = halos[b][group + s, :, lanes_of(0)]
                        right = halos[b][group + s, :, lanes_of(block.col_tiles - 1)]
                    else:
                        continue
                    for o in range(len(outs)):
                        face = lax.select(even, right, left) if o == 0 else lax.select(even, left, right)
                        by = lax.rem(COLS * s + (move if o == 0 else back), LANE)
                        made[o] = jnp.where(slot == s, pltpu.roll(face, by, 1), made[o])
                for o, out in enumerate(outs):
                    out[at] = made[o]
                at += 1


def put(buffer, at, value):
    rows, cols = value.shape
    for rt in range(rows // SUB):
        for ct in range(cols // LANE):
            buffer[at] = value[rows_of(rt), lanes_of(ct)]
            at += 1
    return at


def take(read, at, rows, cols):
    tiles = [
        jnp.concatenate(
            [read(at + rt * (cols // LANE) + ct) for ct in range(cols // LANE)], axis=1
        )
        for rt in range(rows // SUB)
    ]
    return jnp.concatenate(tiles, axis=0), at + (rows // SUB) * (cols // LANE)


def slope(value, dim):
    size = value.shape[dim]
    return pltpu.roll(value, size - 1, dim) - pltpu.roll(value, 1, dim)


def signed(index, inner, total):
    return jnp.where(index < (inner + total) // 2, index, index - total)


def transfer(fine, coarse, halo, down):
    shape = (coarse + halo, fine + halo)
    c = signed(iota(shape, 0), coarse, coarse + halo)
    f = signed(iota(shape, 1), fine, fine + halo)
    half = jnp.right_shift(f, 1)
    if down:
        return jnp.where(half == c, 0.5, 0.0)
    other = half - 1 + 2 * jnp.bitwise_and(f, 1)
    return jnp.where(half == c, 0.75, 0.0) + jnp.where(other == c, 0.25, 0.0)


def exact_dot(a, b, dims):
    return lax.dot_general(
        a, b, (dims, ((), ())), precision=lax.Precision.HIGHEST, preferred_element_type=jnp.float32
    )


def restrict(planes, fine, coarse):
    rows = fine.wide[0]
    by_x = transfer(fine.cols, coarse.cols, LANE, True)
    by_y = transfer(fine.rows, coarse.rows, SUB, True)
    stacked = exact_dot(jnp.concatenate(planes, axis=0), by_x, ((1,), (1,)))
    return [
        exact_dot(by_y, stacked[i * rows : i * rows + rows], ((1,), (0,))) for i in range(3)
    ]


def prolong(planes, fine, coarse):
    rows = coarse.wide[0]
    by_x = transfer(fine.cols, coarse.cols, LANE, False)
    by_y = transfer(fine.rows, coarse.rows, SUB, False)
    stacked = exact_dot(jnp.concatenate(planes, axis=0), by_x, ((1,), (0,)))
    return [
        exact_dot(by_y, stacked[i * rows : i * rows + rows], ((0,), (0,))) for i in range(3)
    ]


def clamp(plane, coarse):
    for axis, dim, inner in (("gy", 0, coarse.rows), ("gx", 1, coarse.cols)):
        spot, count = lax.axis_index(axis), lax.axis_size(axis)
        index = signed(iota(plane.shape, dim), inner, plane.shape[dim])
        low = lax.slice_in_dim(plane, 0, 1, axis=dim)
        high = lax.slice_in_dim(plane, inner - 1, inner, axis=dim)
        least = lax.select(spot == 0, jnp.int32(0), jnp.int32(-plane.shape[dim]))
        most = lax.select(spot == count - 1, jnp.int32(inner - 1), jnp.int32(plane.shape[dim]))
        plane = jnp.where(index < least, low, jnp.where(index > most, high, plane))
    return plane


def interface_sizes(fine, coarse):
    wide = (coarse.wide[0] // SUB) * (coarse.wide[1] // LANE)
    inner = coarse.row_tiles * coarse.col_tiles
    return wide, inner


def z_tiles(blocks):
    faces = sum(b.row_tiles * b.col_tiles * 9 + b.row_tiles + b.col_tiles for b in blocks)
    wide, inner = interface_sizes(*blocks)
    top = 3 * wide + 3 * inner + 3 * blocks[0].row_tiles * blocks[0].col_tiles
    return max(faces, top, 9 * wide)


def widen(blocks, sources, halos, got, wides):
    even = is_even("gx")
    lane = iota((SUB, LANE), 1)
    shift = lax.select(even, jnp.int32(0), jnp.int32(COLS))
    masks = [
        jnp.bitwise_and(lane + shift, LANE - 1) < COLS,
        jnp.bitwise_and(lane + COLS - shift, LANE - 1) < COLS,
    ]
    start = 0
    for b, block in enumerate(blocks):
        rows, cols = block.rows, block.cols
        for p, plane in enumerate(block.planes):
            wide = wides[b]
            wide[p, 0:rows, 0:cols] = own(sources[b], plane, slice(0, rows), slice(0, cols))
            wide[p, rows:, 0:cols] = halos[b][p]
            s = p % SLOTS
            at = start + (p // SLOTS) * (block.row_tiles + 1)
            for rt in range(block.row_tiles + 1):
                tile = jnp.zeros((SUB, LANE), jnp.float32)
                for o, buffer in enumerate(got):
                    by = shift if o == 0 else COLS - shift
                    moved = pltpu.roll(buffer[at + rt], lax.rem(2 * LANE - COLS * s - by, LANE), 1)
                    tile = tile + jnp.where(masks[o], moved, 0.0)
                wide[p, rows_of(rt), cols:] = tile
        start += block.x_tiles()


def step_kernel(blocks, x_count, *refs):
    sources, rest = named(refs)
    halos = rest[:2]
    got = rest[2 : 2 + x_count]
    steps_out = rest[2 + x_count : 4 + x_count]
    first, second, coefs, coefs_coarse, keep = rest[4 + x_count : 9 + x_count]
    wides = rest[9 + x_count : 11 + x_count]
    stresses = rest[11 + x_count : 13 + x_count]
    starts = rest[13 + x_count : 15 + x_count]
    all_coefs = (coefs, coefs_coarse)
    spot_z, count_z = lax.axis_index("gz"), lax.axis_size("gz")
    even = is_even("gz")
    widen(blocks, sources, halos, got, wides)

    for b, block in enumerate(blocks):
        wide, stress = wides[b], stresses[b]
        layers, rows, cols, inverse = block.layers, block.rows, block.cols, block.inverse_step
        half = count_z * layers // 2

        def field(kind, c, layer):
            return wide[block.index[kind, c, layer]]

        def stretched(layer, inner=False):
            if not block.fine:
                return None
            value = field("m", 0, layer)
            if inner:
                value = value[:rows, :cols]
            return lax.select(spot_z * layers + layer < half, value, jnp.ones_like(value))

        def along_z(below, above, stretch):
            if below is None:
                value = above
            elif above is None:
                value = -below
            else:
                value = above - below
            value = value * inverse
            return value if stretch is None else value * stretch

        for layer in range(layers):
            k = [functools.partial(field, "k", c, layer) for c in range(9)]
            u = [field("u", c, layer) for c in range(3)]
            stretch = stretched(layer)
            dz = [
                along_z(
                    field("u", c, layer - 1) if layer else None,
                    field("u", c, layer + 1) if layer < layers - 1 else None,
                    stretch,
                )
                for c in range(3)
            ]
            nx = slope(u[0], 1) * inverse
            ny = slope(u[1], 0) * inverse
            nz = dz[2]
            stress[XX, layer] = k[0]() * nx + k[6]() * ny + k[7]() * nz
            stress[YY, layer] = k[6]() * nx + k[1]() * ny + k[8]() * nz
            stress[ZZ, layer] = k[7]() * nx + k[8]() * ny + k[2]() * nz
            stress[YZ, layer] = k[3]() * (dz[1] + slope(u[2], 0) * inverse)
            stress[XZ, layer] = k[4]() * (dz[0] + slope(u[2], 1) * inverse)
            stress[XY, layer] = k[5]() * ((slope(u[0], 0) + slope(u[1], 1)) * inverse)

        for side, layer in enumerate((0, layers - 1)):
            stretch = stretched(layer)
            for i, c in enumerate((4, 3, 2, 7, 8)):
                value = field("k", c, layer) * inverse
                all_coefs[b][side, i] = value if stretch is None else value * stretch

        table = ((XX, XY, XZ), (XY, YY, YZ), (XZ, YZ, ZZ))
        for layer in range(layers):
            depth = block.depth(layer)
            stretch = stretched(layer, depth >= 2)
            for c in range(3):
                part = table[c]
                height, width = (slice(0, None),) * 2 if depth < 2 else (slice(0, rows), slice(0, cols))
                dx = slope(stress[part[0], layer, height, :], 1)[:, width] * inverse
                dy = slope(stress[part[1], layer, :, width], 0)[height] * inverse
                dz = along_z(
                    stress[part[2], layer - 1, height, width] if layer else None,
                    stress[part[2], layer + 1, height, width] if layer < layers - 1 else None,
                    stretch,
                )
                if depth < 2:
                    now, prev = field("u", c, layer), field("p", c, layer)
                    density = field("d", 0, layer)
                    density = jnp.where(density > 0, density, 1.0)
                else:
                    now = sources[b]["u"][c, layer]
                    prev = sources[b]["p"][c, layer]
                    density = sources[b]["d"][layer]
                value = (2.0 * now - prev) + ALPHA * (dx + dy + dz) / density
                steps_out[b][c, layer] = value[:rows, :cols]
                if depth == 0:
                    starts[b][c] = value
                elif depth == 1 and block.fine:
                    keep[c] = value
                elif depth == 1:
                    starts[b][3 + c] = value

    fine, coarse = blocks
    for i, c in enumerate((4, 3, 2)):
        keep[3 + i] = wides[0][fine.index["k", c, fine.layers - 1]]

    at = 0
    lane = iota((SUB, LANE), 1)

    def send(tile_low, tile_high):
        nonlocal at
        first[at] = lax.select(even, tile_high, tile_low)
        second[at] = lax.select(even, tile_low, tile_high)
        at += 1

    for b, block in enumerate(blocks):
        last = block.layers - 1
        rows, cols = block.rows, block.cols
        for rt in range(block.row_tiles):
            for ct in range(block.col_tiles):
                spot = (rows_of(rt), lanes_of(ct))
                for c in range(3):
                    send(sources[b]["u"][(c, 0) + spot], sources[b]["u"][(c, last) + spot])
                for kind in (XZ, YZ, ZZ):
                    send(stresses[b][(kind, 0) + spot], stresses[b][(kind, last) + spot])
                for i in range(3):
                    send(all_coefs[b][(0, i) + spot], all_coefs[b][(1, i) + spot])
        for ct in range(block.col_tiles):
            for c in range(3):
                low = block.index["u", c, 0]
                high = block.index["u", c, last]
                for edge, to in ((rows, c), (rows + SUB - 1, 4 + c)):
                    one = wides[b][low, edge : edge + 1, lanes_of(ct)]
                    two = wides[b][high, edge : edge + 1, lanes_of(ct)]
                    first[at, to : to + 1] = lax.select(even, two, one)
                    second[at, to : to + 1] = lax.select(even, one, two)
            at += 1
        for rt in range(block.row_tiles):
            pair = [jnp.zeros((SUB, LANE), jnp.float32)] * 2
            for c in range(3):
                for side, layer in enumerate((0, last)):
                    halo = wides[b][block.index["u", c, layer], rows_of(rt), cols:]
                    pair[side] = jnp.where(
                        jnp.right_shift(lane, 1) == c, pltpu.roll(halo, 1 + 2 * c, 1), pair[side]
                    )
            send(*pair)

    @pl.when(spot_z == count_z - 1)
    def _():
        at = 0
        down = restrict([starts[0][c] for c in range(3)], fine, coarse)
        for plane in down:
            at = put(second, at, plane)
        down = restrict([keep[c] for c in range(3)], fine, coarse)
        for plane in down:
            at = put(second, at, plane[: coarse.rows, : coarse.cols])
        for c in range(3):
            at = put(second, at, keep[3 + c][: fine.rows, : fine.cols])

    @pl.when(spot_z == 0)
    def _():
        wide, _ = interface_sizes(fine, coarse)
        for i, c in enumerate((4, 3, 2)):
            k = wides[1][coarse.index["k", c, 0]]
            start, below = starts[1][i], starts[1][3 + i]
            put(second, wide * i, k * (below - start) * 0.25)
            put(second, wide * (3 + i), k * (below - 0.5 * start) * 0.25)
            put(second, wide * (6 + i), k * 0.125)


def last_kernel(blocks, *refs):
    (step_f, step_c, coef_f, coef_c, got_first, got_second, sent, keep) = refs[:8]
    now_f, now_c, metric, density_f, density_c = refs[8:13]
    outs = refs[13:15]
    fine, coarse = blocks
    spot_z, count_z = lax.axis_index("gz"), lax.axis_size("gz")
    even = is_even("gz")
    inside = (spot_z > 0, spot_z < count_z - 1)
    lane = iota((SUB, LANE), 1)

    def reader(side):
        def read(at):
            one, two = got_first[at], got_second[at]
            value = lax.select(even, two, one) if side == 0 else lax.select(even, one, two)
            return lax.select(inside[side], value, jnp.zeros_like(value))

        return read

    start = 0
    for b, block in enumerate(blocks):
        rows, cols, layers, inverse = block.rows, block.cols, block.layers, block.inverse_step
        half = count_z * layers // 2
        now = (now_f, now_c)[b]
        step = (step_f, step_c)[b]
        density = (density_f, density_c)[b]
        coef = (coef_f, coef_c)[b]
        out = outs[b]
        extra = {}

        def add(c, layer, value):
            extra[c, layer] = extra[c, layer] + value if (c, layer) in extra else value

        def stretched(layer, value):
            value = value * inverse
            if not block.fine:
                return value
            factor = metric[layer]
            factor = lax.select(
                spot_z * layers + layer < half, factor, jnp.ones_like(factor)
            )
            return value * factor

        for side, layer, inner in ((0, 0, 1), (1, layers - 1, layers - 2)):
            read = reader(side)
            sign = -1.0 if side == 0 else 1.0
            tiles = block.row_tiles * block.col_tiles

            def plane(k):
                return jnp.concatenate(
                    [
                        jnp.concatenate(
                            [
                                read(start + 9 * (rt * block.col_tiles + ct) + k)
                                for ct in range(block.col_tiles)
                            ],
                            axis=1,
                        )
                        for rt in range(block.row_tiles)
                    ],
                    axis=0,
                )

            row = iota((SUB, LANE), 0)
            beyond = []
            for c in range(3):
                edges = []
                for ct in range(block.col_tiles):
                    tile = read(start + 9 * tiles + ct)
                    ahead = pltpu.roll(tile, (SUB - c) % SUB, 0)
                    behind = pltpu.roll(tile, 3 - c, 0)
                    edges.append(
                        jnp.where(row == 0, ahead, jnp.where(row == SUB - 1, behind, 0.0))
                    )
                sides = []
                for rt in range(block.row_tiles):
                    tile = read(start + 9 * tiles + block.col_tiles + rt)
                    tile = pltpu.roll(tile, LANE - 1 - 2 * c, 1)
                    sides.append(jnp.where((lane == 0) | (lane == LANE - 1), tile, 0.0))
                sides.append(jnp.zeros((SUB, LANE), jnp.float32))
                left = jnp.concatenate(
                    [plane(c), jnp.concatenate(edges, axis=1)], axis=0
                )
                beyond.append(
                    sign * jnp.concatenate([left, jnp.concatenate(sides, axis=0)], axis=1)
                )
            d_xz = coef[side, 0] * beyond[0]
            d_yz = coef[side, 1] * beyond[1]
            d_zz = coef[side, 2] * beyond[2]
            d_xx = coef[side, 3] * beyond[2]
            d_yy = coef[side, 4] * beyond[2]
            add(0, layer, slope(d_xx, 1)[:rows, :cols] * inverse)
            add(1, layer, slope(d_yy, 0)[:rows, :cols] * inverse)
            add(2, layer, (slope(d_xz, 1) + slope(d_yz, 0))[:rows, :cols] * inverse)
            for c, change in enumerate((d_xz, d_yz, d_zz)):
                there = plane(3 + c) - sign * plane(6 + c) * now[c, layer]
                add(c, layer, stretched(layer, sign * there))
                add(c, inner, stretched(inner, sign * change[:rows, :cols]))
        for layer in range(layers):
            for c in range(3):
                value = step[c, layer]
                if (c, layer) in extra:
                    value = value + ALPHA * extra[c, layer] / density[layer]
                out[c, layer] = value
        start += 9 * block.row_tiles * block.col_tiles + block.row_tiles + block.col_tiles

    wide, inner = interface_sizes(fine, coarse)
    height, width = coarse.wide

    @pl.when(spot_z == count_z - 1)
    def _():
        read = lambda at: got_second[at]
        part = [take(read, wide * i, height, width)[0] for i in range(9)]
        above = [keep[c] for c in range(3)]
        k = [jnp.where(keep[3 + c] > 0, keep[3 + c], 1.0) for c in range(3)]
        raised = prolong([clamp(part[c], coarse) for c in range(3)], fine, coarse)
        down = restrict([above[c] + raised[c] / k[c] for c in range(3)], fine, coarse)
        tractions = [clamp(part[3 + c] - part[6 + c] * down[c], coarse) for c in range(3)]
        raised = prolong(tractions, fine, coarse)
        for c in range(3):
            value = above[c] + raised[c] / k[c]
            outs[0][c, fine.layers - 1] = value[: fine.rows, : fine.cols]

    @pl.when(spot_z == 0)
    def _():
        read = lambda at: got_second[at]
        mine = lambda at: sent[at]
        tractions = []
        for c in range(3):
            down = take(read, wide * c, height, width)[0]
            part = take(mine, wide * (3 + c), height, width)[0]
            k = take(mine, wide * (6 + c), height, width)[0]
            tractions.append(clamp(part - k * down, coarse))
        raised = prolong(tractions, fine, coarse)
        at = 3 * wide + 3 * inner
        shares = []
        for c in range(3):
            k, at = take(read, at, fine.rows, fine.cols)
            share = raised[c][: fine.rows, : fine.cols] / k
            share = jnp.concatenate(
                [share, jnp.zeros((SUB, fine.cols), jnp.float32)], axis=0
            )
            shares.append(
                jnp.concatenate(
                    [share, jnp.zeros((fine.wide[0], LANE), jnp.float32)], axis=1
                )
            )
        down = restrict(shares, fine, coarse)
        for c in range(3):
            above = take(read, 3 * wide + inner * c, coarse.rows, coarse.cols)[0]
            total = above + down[c][: coarse.rows, : coarse.cols]
            outs[1][c, 0] = 0.5 * (step_c[c, 0] + total)


def pair_tables(count):
    even = [(i, i + 1) for i in range(0, count - 1, 2)]
    odd = [(i, i + 1) for i in range(1, count - 1, 2)]
    both = lambda some: some + [(b, a) for a, b in some]
    return both(even), both(odd)


def f32(*shape):
    return jax.ShapeDtypeStruct(shape, jnp.float32)


def kernel(body, out_shape, count, scratch=()):
    space = pl.BlockSpec(memory_space=pltpu.VMEM)
    return pl.pallas_call(
        body,
        out_shape=out_shape,
        in_specs=[space] * count,
        out_specs=[space] * len(out_shape),
        scratch_shapes=[pltpu.VMEM(shape, jnp.float32) for shape in scratch],
    )


def per_device(
    fine_now,
    fine_prev,
    stiffness,
    metric,
    density,
    coarse_now,
    coarse_prev,
    coarse_stiffness,
    coarse_density,
):
    blocks = fine, coarse = (
        Block(fine_now.shape[1:], True),
        Block(coarse_now.shape[1:], False),
    )
    arrays = [
        fine_now, stiffness, metric, fine_prev, density,
        coarse_now, coarse_stiffness, coarse_prev, coarse_density,
    ]
    count_z = lax.axis_size("gz")
    assert count_z % 2 == 0

    _, row_count = row_table(blocks)
    sent = kernel(functools.partial(rows_kernel, blocks), [f32(row_count, LANE)] * 2, 9)(*arrays)
    by_row = [
        lax.ppermute(buffer, "gy", pairs) if pairs else jnp.zeros_like(buffer)
        for buffer, pairs in zip(sent, pair_tables(lax.axis_size("gy")))
    ]

    tables = [pairs for pairs in pair_tables(lax.axis_size("gx")) if pairs]
    tiles = sum(block.x_tiles() for block in blocks)
    halo_shapes = [f32(len(block.planes), SUB, block.cols) for block in blocks]
    made = kernel(
        functools.partial(columns_kernel, blocks, len(tables)),
        halo_shapes + [f32(tiles, SUB, LANE)] * len(tables),
        11,
    )(*arrays, *by_row)
    halos = made[:2]
    by_column = [
        lax.ppermute(buffer, "gx", pairs) for buffer, pairs in zip(made[2:], tables)
    ]

    z_shape = f32(z_tiles(blocks), SUB, LANE)
    step_f, step_c, first, second, coef_f, coef_c, keep = kernel(
        functools.partial(step_kernel, blocks, len(tables)),
        [f32(*fine_now.shape), f32(*coarse_now.shape), z_shape, z_shape]
        + [f32(2, 5, *block.wide) for block in blocks]
        + [f32(6, *fine.wide)],
        11 + len(tables),
        [(len(block.planes), *block.wide) for block in blocks]
        + [(6, block.layers, *block.wide) for block in blocks]
        + [(3, *fine.wide), (6, *coarse.wide)],
    )(*arrays, *halos, *by_column)
    even_pairs, odd_pairs = pair_tables(count_z)
    odd_pairs = odd_pairs + [(0, count_z - 1), (count_z - 1, 0)]
    got_first = lax.ppermute(first, "gz", even_pairs)
    got_second = lax.ppermute(second, "gz", odd_pairs)

    return tuple(
        kernel(
            functools.partial(last_kernel, blocks),
            [f32(*fine_now.shape), f32(*coarse_now.shape)],
            13,
        )(
            step_f, step_c, coef_f, coef_c, got_first, got_second, second, keep,
            fine_now, coarse_now, metric, density, coarse_density,
        )
    )


def solution(mesh):
    block = P(None, "gz", "gy", "gx")
    field = P("gz", "gy", "gx")
    return jax.shard_map(
        per_device,
        mesh=mesh,
        in_specs=(block, block, block, field, field, block, block, block, field),
        out_specs=(block, block),
        check_vma=False,
    )
```

```python
import functools

import numpy as np
import jax
import jax.numpy as jnp
from jax import lax
from jax.experimental import pallas as pl
from jax.experimental.pallas import tpu as pltpu
from jax.sharding import PartitionSpec as P

ITERS = 3
TIME_STEP = 0.2
ALPHA = TIME_STEP * TIME_STEP
SUB = 8
VMEM_BYTES = 16 * 2**20
LANE = 128
COLS = 4
SLOTS = LANE // COLS
Y_CHANNELS = (1, 3, 5, 6, 8)
Z_CHANNELS = (2, 3, 4, 7, 8)
XX, YY, ZZ, YZ, XZ, XY = range(6)


class Block:
    def __init__(self, shape, fine):
        self.layers, self.rows, self.cols = shape
        self.fine = fine
        self.inverse_step = 0.5 if fine else 0.25
        self.wide = (self.rows + SUB, self.cols + LANE)
        self.row_tiles, self.col_tiles = self.rows // SUB, self.cols // LANE
        self.planes = []
        for layer in range(self.layers):
            depth = self.depth(layer)
            for c in range(3):
                self.planes.append(("u", c, layer, 2, (2, 2, 1)[depth] if depth < 3 else 0))
            for c in range(9):
                base = 1 if c in Y_CHANNELS else 0
                extra = 2 if depth < 2 else (2 - base if depth == 2 and c in Z_CHANNELS else 0)
                self.planes.append(("k", c, layer, base, extra))
            if fine:
                self.planes.append(("m", 0, layer, 1, 0))
            if depth < 2:
                for c in range(3):
                    self.planes.append(("p", c, layer, 0, 2))
                self.planes.append(("d", 0, layer, 0, 2))
        self.index = {plane[:3]: i for i, plane in enumerate(self.planes)}

    def depth(self, layer):
        return self.layers - 1 - layer if self.fine else layer

    def x_tiles(self):
        return -(-len(self.planes) // SLOTS) * (self.row_tiles + 1)


def row_table(blocks):
    base, extra, at = {}, {}, 0
    for count in (2, 1):
        for b, block in enumerate(blocks):
            for p, plane in enumerate(block.planes):
                if plane[3] == count:
                    for t in range(block.col_tiles):
                        base[b, p, t] = slice(at, at + count)
                        at += count
    start, ends = at, []
    for b, block in enumerate(blocks):
        at = start
        for count in (2, 1):
            for p, plane in enumerate(block.planes):
                if plane[4] == count:
                    for t in range(block.col_tiles):
                        extra[b, p, t] = slice(at, at + count)
                        at += count
        ends.append(at)
    return base, extra, -(-max(ends) // SUB) * SUB


def lanes_of(t):
    return slice(LANE * t, LANE * t + LANE)


def rows_of(t):
    return slice(SUB * t, SUB * t + SUB)


def own(refs, plane, rows, lanes):
    kind, c, layer = plane[:3]
    if kind in ("m", "d"):
        return refs[kind][layer, rows, lanes]
    return refs[kind][c, layer, rows, lanes]


def is_even(axis):
    return lax.rem(lax.axis_index(axis), 2) == 0


def iota(shape, dim):
    return lax.broadcasted_iota(jnp.int32, shape, dim)


def named(refs):
    fine = dict(zip("ukmpd", refs[:5]))
    coarse = dict(zip("ukpd", refs[5:9]))
    return (fine, coarse), refs[9:]


def rows_kernel(blocks, *refs):
    held, loaded, (first, second, done) = refs[:9], refs[9:18], refs[18:]
    copies = [
        pltpu.make_async_copy(source, target, done.at[i])
        for i, (source, target) in enumerate(zip(held, loaded))
    ]
    for copy in copies:
        copy.start()
    for copy in copies:
        copy.wait()
    sources, _ = named(loaded)
    base, extra, _ = row_table(blocks)
    even = is_even("gy")
    is_low = lax.axis_index("gz") == 0

    def move(b, block, plane, at, t, near, far):
        high = own(sources[b], plane, slice(block.rows - far, block.rows - near), lanes_of(t))
        low = own(sources[b], plane, slice(near, far), lanes_of(t))
        first[at, :] = lax.select(even, high, low)
        second[at, :] = lax.select(even, low, high)

    for b, block in enumerate(blocks):
        for p, plane in enumerate(block.planes):
            for t in range(block.col_tiles):
                if plane[3]:
                    move(b, block, plane, base[b, p, t], t, 0, plane[3])
    for b, block in enumerate(blocks):

        @pl.when(is_low != block.fine)
        def _():
            for p, plane in enumerate(block.planes):
                for t in range(block.col_tiles):
                    if plane[4]:
                        move(b, block, plane, extra[b, p, t], t, plane[3], plane[3] + plane[4])


def columns_kernel(blocks, both, *refs):
    sources, rest = named(refs)
    got_first, got_second = rest[:2]
    halos = rest[2:4]
    outs = rest[4:]
    base, extra, _ = row_table(blocks)
    even = is_even("gy")
    is_low = lax.axis_index("gz") == 0

    def place(b, p, at, t, near, far):
        one, two = got_first[at, :], got_second[at, :]
        halos[b][p, near:far, lanes_of(t)] = lax.select(even, one, two)
        halos[b][p, SUB - far : SUB - near, lanes_of(t)] = lax.select(even, two, one)

    for b, block in enumerate(blocks):
        for p, plane in enumerate(block.planes):
            halos[b][p] = jnp.zeros((SUB, block.cols), jnp.float32)
            for t in range(block.col_tiles):
                if plane[3]:
                    place(b, p, base[b, p, t], t, 0, plane[3])
    for b, block in enumerate(blocks):

        @pl.when(is_low != block.fine)
        def _():
            for p, plane in enumerate(block.planes):
                for t in range(block.col_tiles):
                    if plane[4]:
                        place(b, p, extra[b, p, t], t, plane[3], plane[3] + plane[4])

    even = is_even("gx")
    lane = iota((SUB, LANE), 1)
    slot = lax.shift_right_logical(lane, jnp.full((SUB, LANE), 2, jnp.int32))
    move = lax.select(even, jnp.int32(COLS), jnp.int32(0))
    back = COLS - move
    at = 0
    for b, block in enumerate(blocks):
        for group in range(0, len(block.planes), SLOTS):
            for rt in range(block.row_tiles + 1):
                made = [jnp.zeros((SUB, LANE), jnp.float32) for _ in outs]
                for s, plane in enumerate(block.planes[group : group + SLOTS]):
                    if rt < block.row_tiles:
                        left = own(sources[b], plane, rows_of(rt), lanes_of(0))
                        right = own(sources[b], plane, rows_of(rt), lanes_of(block.col_tiles - 1))
                    elif plane[3] + plane[4]:
                        left = halos[b][group + s, :, lanes_of(0)]
                        right = halos[b][group + s, :, lanes_of(block.col_tiles - 1)]
                    else:
                        continue
                    for o in range(len(outs)):
                        face = lax.select(even, right, left) if o == 0 else lax.select(even, left, right)
                        by = lax.rem(COLS * s + (move if o == 0 else back), LANE)
                        made[o] = jnp.where(slot == s, pltpu.roll(face, by, 1), made[o])
                for o, out in enumerate(outs):
                    out[at] = made[o]
                at += 1


def put(buffer, at, value):
    rows, cols = value.shape
    for rt in range(rows // SUB):
        for ct in range(cols // LANE):
            buffer[at] = value[rows_of(rt), lanes_of(ct)]
            at += 1
    return at


def take(read, at, rows, cols):
    tiles = [
        jnp.concatenate(
            [read(at + rt * (cols // LANE) + ct) for ct in range(cols // LANE)], axis=1
        )
        for rt in range(rows // SUB)
    ]
    return jnp.concatenate(tiles, axis=0), at + (rows // SUB) * (cols // LANE)


def slope(value, dim):
    size = value.shape[dim]
    return pltpu.roll(value, size - 1, dim) - pltpu.roll(value, 1, dim)


def signed(index, inner, total):
    return jnp.where(index < (inner + total) // 2, index, index - total)


def transfer(fine, coarse, halo, down):
    shape = (coarse + halo, fine + halo)
    c = signed(iota(shape, 0), coarse, coarse + halo)
    f = signed(iota(shape, 1), fine, fine + halo)
    half = jnp.right_shift(f, 1)
    if down:
        return jnp.where(half == c, 0.5, 0.0)
    other = half - 1 + 2 * jnp.bitwise_and(f, 1)
    return jnp.where(half == c, 0.75, 0.0) + jnp.where(other == c, 0.25, 0.0)


def exact_dot(a, b, dims):
    return lax.dot_general(
        a, b, (dims, ((), ())), precision=lax.Precision.HIGHEST, preferred_element_type=jnp.float32
    )


def restrict(planes, fine, coarse):
    rows = fine.wide[0]
    by_x = transfer(fine.cols, coarse.cols, LANE, True)
    by_y = transfer(fine.rows, coarse.rows, SUB, True)
    stacked = exact_dot(jnp.concatenate(planes, axis=0), by_x, ((1,), (1,)))
    return [
        exact_dot(by_y, stacked[i * rows : i * rows + rows], ((1,), (0,))) for i in range(3)
    ]


def prolong(planes, fine, coarse):
    rows = coarse.wide[0]
    by_x = transfer(fine.cols, coarse.cols, LANE, False)
    by_y = transfer(fine.rows, coarse.rows, SUB, False)
    stacked = exact_dot(jnp.concatenate(planes, axis=0), by_x, ((1,), (0,)))
    return [
        exact_dot(by_y, stacked[i * rows : i * rows + rows], ((0,), (0,))) for i in range(3)
    ]


def clamp(plane, coarse):
    for axis, dim, inner in (("gy", 0, coarse.rows), ("gx", 1, coarse.cols)):
        spot, count = lax.axis_index(axis), lax.axis_size(axis)
        index = signed(iota(plane.shape, dim), inner, plane.shape[dim])
        low = lax.slice_in_dim(plane, 0, 1, axis=dim)
        high = lax.slice_in_dim(plane, inner - 1, inner, axis=dim)
        least = lax.select(spot == 0, jnp.int32(0), jnp.int32(-plane.shape[dim]))
        most = lax.select(spot == count - 1, jnp.int32(inner - 1), jnp.int32(plane.shape[dim]))
        plane = jnp.where(index < least, low, jnp.where(index > most, high, plane))
    return plane


def wide_tiles(count, coarse):
    inner = coarse.row_tiles * coarse.col_tiles
    return count * inner + -(-count // 2) * coarse.col_tiles + coarse.row_tiles + 1


def put_wide(buffer, at, planes, coarse):
    rows, cols = coarse.rows, coarse.cols
    for value in planes:
        at = put(buffer, at, value[:rows, :cols])
    for ct in range(coarse.col_tiles):
        for i, value in enumerate(planes):
            to = 4 * (i % 2)
            buffer[at + i // 2, to : to + 2] = value[rows : rows + 2, lanes_of(ct)]
            buffer[at + i // 2, to + 2 : to + 4] = value[rows + SUB - 2 :, lanes_of(ct)]
        at += -(-len(planes) // 2)
    slot = jnp.right_shift(iota((SUB, LANE), 1), 2)
    for rt in range(coarse.row_tiles + 1):
        tile = jnp.zeros((SUB, LANE), jnp.float32)
        for i, value in enumerate(planes):
            tile = jnp.where(slot == i, pltpu.roll(value[rows_of(rt), cols:], 2 + 4 * i, 1), tile)
        buffer[at] = tile
        at += 1
    return at


def take_wide(buffer, at, count, coarse):
    row, lane = iota((SUB, LANE), 0), iota((SUB, LANE), 1)
    read = lambda spot: buffer[spot]
    inner = []
    for _ in range(count):
        value, at = take(read, at, coarse.rows, coarse.cols)
        inner.append(value)
    ends = [[] for _ in range(count)]
    for ct in range(coarse.col_tiles):
        for i in range(count):
            tile = buffer[at + i // 2]
            start = 4 * (i % 2)
            ahead = pltpu.roll(tile, (SUB - start) % SUB, 0)
            behind = pltpu.roll(tile, 4 - start, 0)
            ends[i].append(jnp.where(row < 2, ahead, jnp.where(row >= SUB - 2, behind, 0.0)))
        at += -(-count // 2)
    sides = [[] for _ in range(count)]
    for rt in range(coarse.row_tiles + 1):
        for i in range(count):
            tile = pltpu.roll(buffer[at], LANE - 2 - 4 * i, 1)
            sides[i].append(jnp.where((lane < 2) | (lane >= LANE - 2), tile, 0.0))
        at += 1
    planes = []
    for i in range(count):
        left = jnp.concatenate([inner[i], jnp.concatenate(ends[i], axis=1)], axis=0)
        planes.append(jnp.concatenate([left, jnp.concatenate(sides[i], axis=0)], axis=1))
    return planes, at


def interface_tiles(fine, coarse):
    top = wide_tiles(3, coarse) + 3 * coarse.row_tiles * coarse.col_tiles
    return max(top + 3 * fine.row_tiles * fine.col_tiles, wide_tiles(9, coarse))


def face_tiles(blocks):
    return sum(b.row_tiles * b.col_tiles * 9 + b.row_tiles + b.col_tiles for b in blocks)


def widen(blocks, sources, halos, got, wides):
    even = is_even("gx")
    lane = iota((SUB, LANE), 1)
    shift = lax.select(even, jnp.int32(0), jnp.int32(COLS))
    masks = [
        jnp.bitwise_and(lane + shift, LANE - 1) < COLS,
        jnp.bitwise_and(lane + COLS - shift, LANE - 1) < COLS,
    ]
    start = 0
    for b, block in enumerate(blocks):
        rows, cols = block.rows, block.cols
        for p, plane in enumerate(block.planes):
            wide = wides[b]
            wide[p, 0:rows, 0:cols] = own(sources[b], plane, slice(0, rows), slice(0, cols))
            wide[p, rows:, 0:cols] = halos[b][p]
            s = p % SLOTS
            at = start + (p // SLOTS) * (block.row_tiles + 1)
            for rt in range(block.row_tiles + 1):
                tile = jnp.zeros((SUB, LANE), jnp.float32)
                for o, buffer in enumerate(got):
                    by = shift if o == 0 else COLS - shift
                    moved = pltpu.roll(buffer[at + rt], lax.rem(2 * LANE - COLS * s - by, LANE), 1)
                    tile = tile + jnp.where(masks[o], moved, 0.0)
                wide[p, rows_of(rt), cols:] = tile
        start += block.x_tiles()


def step_kernel(blocks, x_count, *refs):
    sources, rest = named(refs)
    halos = rest[:2]
    got = rest[2 : 2 + x_count]
    steps_out = rest[2 + x_count : 4 + x_count]
    first, second, third, coefs, coefs_coarse, keep = rest[4 + x_count : 10 + x_count]
    wides = rest[10 + x_count : 12 + x_count]
    stresses = rest[12 + x_count : 14 + x_count]
    starts = rest[14 + x_count : 16 + x_count]
    all_coefs = (coefs, coefs_coarse)
    spot_z, count_z = lax.axis_index("gz"), lax.axis_size("gz")
    even = is_even("gz")
    widen(blocks, sources, halos, got, wides)

    for b, block in enumerate(blocks):
        wide, stress = wides[b], stresses[b]
        layers, rows, cols, inverse = block.layers, block.rows, block.cols, block.inverse_step
        half = count_z * layers // 2

        def field(kind, c, layer):
            return wide[block.index[kind, c, layer]]

        def stretched(layer, inner=False):
            if not block.fine:
                return None
            value = field("m", 0, layer)
            if inner:
                value = value[:rows, :cols]
            return lax.select(spot_z * layers + layer < half, value, jnp.ones_like(value))

        def along_z(below, above, stretch):
            if below is None:
                value = above
            elif above is None:
                value = -below
            else:
                value = above - below
            value = value * inverse
            return value if stretch is None else value * stretch

        for layer in range(layers):
            k = [functools.partial(field, "k", c, layer) for c in range(9)]
            u = [field("u", c, layer) for c in range(3)]
            stretch = stretched(layer)
            dz = [
                along_z(
                    field("u", c, layer - 1) if layer else None,
                    field("u", c, layer + 1) if layer < layers - 1 else None,
                    stretch,
                )
                for c in range(3)
            ]
            nx = slope(u[0], 1) * inverse
            ny = slope(u[1], 0) * inverse
            nz = dz[2]
            stress[XX, layer] = k[0]() * nx + k[6]() * ny + k[7]() * nz
            stress[YY, layer] = k[6]() * nx + k[1]() * ny + k[8]() * nz
            stress[ZZ, layer] = k[7]() * nx + k[8]() * ny + k[2]() * nz
            stress[YZ, layer] = k[3]() * (dz[1] + slope(u[2], 0) * inverse)
            stress[XZ, layer] = k[4]() * (dz[0] + slope(u[2], 1) * inverse)
            stress[XY, layer] = k[5]() * ((slope(u[0], 0) + slope(u[1], 1)) * inverse)

        for side, layer in enumerate((0, layers - 1)):
            stretch = stretched(layer)
            for i, c in enumerate((4, 3, 2, 7, 8)):
                value = field("k", c, layer) * inverse
                all_coefs[b][side, i] = value if stretch is None else value * stretch

        table = ((XX, XY, XZ), (XY, YY, YZ), (XZ, YZ, ZZ))
        for layer in range(layers):
            depth = block.depth(layer)
            stretch = stretched(layer, depth >= 2)
            for c in range(3):
                part = table[c]
                height, width = (slice(0, None),) * 2 if depth < 2 else (slice(0, rows), slice(0, cols))
                dx = slope(stress[part[0], layer, height, :], 1)[:, width] * inverse
                dy = slope(stress[part[1], layer, :, width], 0)[height] * inverse
                dz = along_z(
                    stress[part[2], layer - 1, height, width] if layer else None,
                    stress[part[2], layer + 1, height, width] if layer < layers - 1 else None,
                    stretch,
                )
                if depth < 2:
                    now, prev = field("u", c, layer), field("p", c, layer)
                    density = field("d", 0, layer)
                    density = jnp.where(density > 0, density, 1.0)
                else:
                    now = sources[b]["u"][c, layer]
                    prev = sources[b]["p"][c, layer]
                    density = sources[b]["d"][layer]
                value = (2.0 * now - prev) + ALPHA * (dx + dy + dz) / density
                steps_out[b][c, layer] = value[:rows, :cols]
                if depth == 0:
                    starts[b][c] = value
                elif depth == 1 and block.fine:
                    keep[c] = value
                elif depth == 1:
                    starts[b][3 + c] = value

    fine, coarse = blocks
    for i, c in enumerate((4, 3, 2)):
        keep[3 + i] = wides[0][fine.index["k", c, fine.layers - 1]]

    at = 0
    lane = iota((SUB, LANE), 1)

    def send(tile_low, tile_high):
        nonlocal at
        first[at] = lax.select(even, tile_high, tile_low)
        second[at] = lax.select(even, tile_low, tile_high)
        at += 1

    for b, block in enumerate(blocks):
        last = block.layers - 1
        rows, cols = block.rows, block.cols
        for rt in range(block.row_tiles):
            for ct in range(block.col_tiles):
                spot = (rows_of(rt), lanes_of(ct))
                for c in range(3):
                    send(sources[b]["u"][(c, 0) + spot], sources[b]["u"][(c, last) + spot])
                for kind in (XZ, YZ, ZZ):
                    send(stresses[b][(kind, 0) + spot], stresses[b][(kind, last) + spot])
                for i in range(3):
                    send(all_coefs[b][(0, i) + spot], all_coefs[b][(1, i) + spot])
        for ct in range(block.col_tiles):
            for c in range(3):
                low = block.index["u", c, 0]
                high = block.index["u", c, last]
                for edge, to in ((rows, c), (rows + SUB - 1, 4 + c)):
                    one = wides[b][low, edge : edge + 1, lanes_of(ct)]
                    two = wides[b][high, edge : edge + 1, lanes_of(ct)]
                    first[at, to : to + 1] = lax.select(even, two, one)
                    second[at, to : to + 1] = lax.select(even, one, two)
            at += 1
        for rt in range(block.row_tiles):
            pair = [jnp.zeros((SUB, LANE), jnp.float32)] * 2
            for c in range(3):
                for side, layer in enumerate((0, last)):
                    halo = wides[b][block.index["u", c, layer], rows_of(rt), cols:]
                    pair[side] = jnp.where(
                        jnp.right_shift(lane, 1) == c, pltpu.roll(halo, 1 + 2 * c, 1), pair[side]
                    )
            send(*pair)

    @pl.when(spot_z == count_z - 1)
    def _():
        down = restrict([starts[0][c] for c in range(3)], fine, coarse)
        at = put_wide(third, 0, down, coarse)
        down = restrict([keep[c] for c in range(3)], fine, coarse)
        for plane in down:
            at = put(third, at, plane[: coarse.rows, : coarse.cols])
        for c in range(3):
            at = put(third, at, keep[3 + c][: fine.rows, : fine.cols])

    @pl.when(spot_z == 0)
    def _():
        planes = [[], [], []]
        for i, c in enumerate((4, 3, 2)):
            k = wides[1][coarse.index["k", c, 0]]
            start, below = starts[1][i], starts[1][3 + i]
            planes[0].append(k * (below - start) * 0.25)
            planes[1].append(k * (below - 0.5 * start) * 0.25)
            planes[2].append(k * 0.125)
        put_wide(third, 0, sum(planes, []), coarse)


def last_kernel(blocks, *refs):
    (step_f, step_c, coef_f, coef_c, got_first, got_second, got_third, sent, keep) = refs[:9]
    now_f, now_c, metric, density_f, density_c = refs[9:14]
    outs = refs[14:16]
    fine, coarse = blocks
    spot_z, count_z = lax.axis_index("gz"), lax.axis_size("gz")
    even = is_even("gz")
    inside = (spot_z > 0, spot_z < count_z - 1)
    lane = iota((SUB, LANE), 1)

    def reader(side):
        def read(at):
            one, two = got_first[at], got_second[at]
            value = lax.select(even, two, one) if side == 0 else lax.select(even, one, two)
            return lax.select(inside[side], value, jnp.zeros_like(value))

        return read

    start = 0
    for b, block in enumerate(blocks):
        rows, cols, layers, inverse = block.rows, block.cols, block.layers, block.inverse_step
        half = count_z * layers // 2
        now = (now_f, now_c)[b]
        step = (step_f, step_c)[b]
        density = (density_f, density_c)[b]
        coef = (coef_f, coef_c)[b]
        out = outs[b]
        extra = {}

        def add(c, layer, value):
            extra[c, layer] = extra[c, layer] + value if (c, layer) in extra else value

        def stretched(layer, value):
            value = value * inverse
            if not block.fine:
                return value
            factor = metric[layer]
            factor = lax.select(
                spot_z * layers + layer < half, factor, jnp.ones_like(factor)
            )
            return value * factor

        for side, layer, inner in ((0, 0, 1), (1, layers - 1, layers - 2)):
            read = reader(side)
            sign = -1.0 if side == 0 else 1.0
            tiles = block.row_tiles * block.col_tiles

            def plane(k):
                return jnp.concatenate(
                    [
                        jnp.concatenate(
                            [
                                read(start + 9 * (rt * block.col_tiles + ct) + k)
                                for ct in range(block.col_tiles)
                            ],
                            axis=1,
                        )
                        for rt in range(block.row_tiles)
                    ],
                    axis=0,
                )

            row = iota((SUB, LANE), 0)
            beyond = []
            for c in range(3):
                edges = []
                for ct in range(block.col_tiles):
                    tile = read(start + 9 * tiles + ct)
                    ahead = pltpu.roll(tile, (SUB - c) % SUB, 0)
                    behind = pltpu.roll(tile, 3 - c, 0)
                    edges.append(
                        jnp.where(row == 0, ahead, jnp.where(row == SUB - 1, behind, 0.0))
                    )
                sides = []
                for rt in range(block.row_tiles):
                    tile = read(start + 9 * tiles + block.col_tiles + rt)
                    tile = pltpu.roll(tile, LANE - 1 - 2 * c, 1)
                    sides.append(jnp.where((lane == 0) | (lane == LANE - 1), tile, 0.0))
                sides.append(jnp.zeros((SUB, LANE), jnp.float32))
                left = jnp.concatenate(
                    [plane(c), jnp.concatenate(edges, axis=1)], axis=0
                )
                beyond.append(
                    sign * jnp.concatenate([left, jnp.concatenate(sides, axis=0)], axis=1)
                )
            d_xz = coef[side, 0] * beyond[0]
            d_yz = coef[side, 1] * beyond[1]
            d_zz = coef[side, 2] * beyond[2]
            d_xx = coef[side, 3] * beyond[2]
            d_yy = coef[side, 4] * beyond[2]
            add(0, layer, slope(d_xx, 1)[:rows, :cols] * inverse)
            add(1, layer, slope(d_yy, 0)[:rows, :cols] * inverse)
            add(2, layer, (slope(d_xz, 1) + slope(d_yz, 0))[:rows, :cols] * inverse)
            for c, change in enumerate((d_xz, d_yz, d_zz)):
                there = plane(3 + c) - sign * plane(6 + c) * now[c, layer]
                add(c, layer, stretched(layer, sign * there))
                add(c, inner, stretched(inner, sign * change[:rows, :cols]))
        for layer in range(layers):
            for c in range(3):
                value = step[c, layer]
                if (c, layer) in extra:
                    value = value + ALPHA * extra[c, layer] / density[layer]
                out[c, layer] = value
        start += 9 * block.row_tiles * block.col_tiles + block.row_tiles + block.col_tiles

    @pl.when(spot_z == count_z - 1)
    def _():
        part, _ = take_wide(got_third, 0, 9, coarse)
        above = [keep[c] for c in range(3)]
        k = [jnp.where(keep[3 + c] > 0, keep[3 + c], 1.0) for c in range(3)]
        raised = prolong([clamp(part[c], coarse) for c in range(3)], fine, coarse)
        down = restrict([above[c] + raised[c] / k[c] for c in range(3)], fine, coarse)
        tractions = [clamp(part[3 + c] - part[6 + c] * down[c], coarse) for c in range(3)]
        raised = prolong(tractions, fine, coarse)
        for c in range(3):
            value = above[c] + raised[c] / k[c]
            outs[0][c, fine.layers - 1] = value[: fine.rows, : fine.cols]

    @pl.when(spot_z == 0)
    def _():
        read = lambda spot: got_third[spot]
        down, at = take_wide(got_third, 0, 3, coarse)
        part, _ = take_wide(sent, 0, 9, coarse)
        tractions = [clamp(part[3 + c] - part[6 + c] * down[c], coarse) for c in range(3)]
        raised = prolong(tractions, fine, coarse)
        above = []
        for c in range(3):
            value, at = take(read, at, coarse.rows, coarse.cols)
            above.append(value)
        shares = []
        for c in range(3):
            k, at = take(read, at, fine.rows, fine.cols)
            share = raised[c][: fine.rows, : fine.cols] / k
            share = jnp.concatenate(
                [share, jnp.zeros((SUB, fine.cols), jnp.float32)], axis=0
            )
            shares.append(
                jnp.concatenate(
                    [share, jnp.zeros((fine.wide[0], LANE), jnp.float32)], axis=1
                )
            )
        down = restrict(shares, fine, coarse)
        for c in range(3):
            total = above[c] + down[c][: coarse.rows, : coarse.cols]
            outs[1][c, 0] = 0.5 * (step_c[c, 0] + total)


def pair_tables(count):
    even = [(i, i + 1) for i in range(0, count - 1, 2)]
    odd = [(i, i + 1) for i in range(1, count - 1, 2)]
    both = lambda some: some + [(b, a) for a, b in some]
    return both(even), both(odd)


def f32(*shape):
    return jax.ShapeDtypeStruct(shape, jnp.float32)


def kernel(body, out_shape, count, scratch=(), held=False):
    space = pl.BlockSpec(memory_space=pltpu.VMEM)
    outside = pl.BlockSpec(memory_space=pltpu.HBM) if held else space
    scratches = [pltpu.VMEM(shape, jnp.float32) for shape in scratch]
    if held:
        scratches = [pltpu.SemaphoreType.DMA((count,))]
    return pl.pallas_call(
        body,
        out_shape=out_shape,
        in_specs=[outside] * count,
        out_specs=[space] * len(out_shape),
        scratch_shapes=scratches,
        compiler_params=pltpu.CompilerParams(vmem_limit_bytes=VMEM_BYTES),
    )


def per_device(
    fine_now,
    fine_prev,
    stiffness,
    metric,
    density,
    coarse_now,
    coarse_prev,
    coarse_stiffness,
    coarse_density,
):
    blocks = fine, coarse = (
        Block(fine_now.shape[1:], True),
        Block(coarse_now.shape[1:], False),
    )
    arrays = [
        fine_now, stiffness, metric, fine_prev, density,
        coarse_now, coarse_stiffness, coarse_prev, coarse_density,
    ]
    count_z = lax.axis_size("gz")
    assert count_z % 2 == 0

    _, _, row_count = row_table(blocks)
    *arrays, first, second = kernel(
        functools.partial(rows_kernel, blocks),
        [f32(*array.shape) for array in arrays] + [f32(row_count, LANE)] * 2,
        len(arrays),
        held=True,
    )(*[pltpu.with_memory_space_constraint(array, pltpu.HBM) for array in arrays])
    by_row = [
        lax.ppermute(buffer, "gy", pairs) if pairs else jnp.zeros_like(buffer)
        for buffer, pairs in zip((first, second), pair_tables(lax.axis_size("gy")))
    ]

    tables = [pairs for pairs in pair_tables(lax.axis_size("gx")) if pairs]
    tiles = sum(block.x_tiles() for block in blocks)
    halo_shapes = [f32(len(block.planes), SUB, block.cols) for block in blocks]
    made = kernel(
        functools.partial(columns_kernel, blocks, len(tables)),
        halo_shapes + [f32(tiles, SUB, LANE)] * len(tables),
        11,
    )(*arrays, *by_row)
    halos = made[:2]
    by_column = [
        lax.ppermute(buffer, "gx", pairs) for buffer, pairs in zip(made[2:], tables)
    ]

    z_shape = f32(face_tiles(blocks), SUB, LANE)
    step_f, step_c, first, second, third, coef_f, coef_c, keep = kernel(
        functools.partial(step_kernel, blocks, len(tables)),
        [f32(*fine_now.shape), f32(*coarse_now.shape), z_shape, z_shape]
        + [f32(interface_tiles(*blocks), SUB, LANE)]
        + [f32(2, 5, *block.wide) for block in blocks]
        + [f32(6, *fine.wide)],
        11 + len(tables),
        [(len(block.planes), *block.wide) for block in blocks]
        + [(6, block.layers, *block.wide) for block in blocks]
        + [(3, *fine.wide), (6, *coarse.wide)],
    )(*arrays, *halos, *by_column)
    even_pairs, odd_pairs = pair_tables(count_z)
    got_first = lax.ppermute(first, "gz", even_pairs)
    got_second = lax.ppermute(second, "gz", odd_pairs) if odd_pairs else jnp.zeros_like(second)
    got_third = lax.ppermute(third, "gz", [(0, count_z - 1), (count_z - 1, 0)])

    now_f, _, metric, _, density = arrays[:5]
    now_c, _, _, density_c = arrays[5:]
    return tuple(
        kernel(
            functools.partial(last_kernel, blocks),
            [f32(*fine_now.shape), f32(*coarse_now.shape)],
            14,
        )(
            step_f, step_c, coef_f, coef_c, got_first, got_second, got_third, third, keep,
            now_f, now_c, metric, density, density_c,
        )
    )


def solution(mesh):
    block = P(None, "gz", "gy", "gx")
    field = P("gz", "gy", "gx")
    return jax.shard_map(
        per_device,
        mesh=mesh,
        in_specs=(block, block, block, field, field, block, block, block, field),
        out_specs=(block, block),
        check_vma=False,
    )
```

```python
import functools

import numpy as np
import jax
import jax.numpy as jnp
from jax import lax
from jax.experimental import pallas as pl
from jax.experimental.pallas import tpu as pltpu
from jax.sharding import PartitionSpec as P

ITERS = 3
TIME_STEP = 0.2
ALPHA = TIME_STEP * TIME_STEP
SUB = 8
VMEM_BYTES = 16 * 2**20
LANE = 128
COLS = 4
SLOTS = LANE // COLS
Y_CHANNELS = (1, 3, 5, 6, 8)
Z_CHANNELS = (2, 3, 4, 7, 8)
XX, YY, ZZ, YZ, XZ, XY = range(6)


class Block:
    def __init__(self, shape, fine):
        self.layers, self.rows, self.cols = shape
        self.fine = fine
        self.inverse_step = 0.5 if fine else 0.25
        self.wide = (self.rows + SUB, self.cols + LANE)
        self.row_tiles, self.col_tiles = self.rows // SUB, self.cols // LANE
        self.planes = []
        for layer in range(self.layers):
            depth = self.depth(layer)
            for c in range(3):
                self.planes.append(("u", c, layer, 2, (2, 2, 1)[depth] if depth < 3 else 0))
            for c in range(9):
                base = 1 if c in Y_CHANNELS else 0
                extra = 2 if depth < 2 else (2 - base if depth == 2 and c in Z_CHANNELS else 0)
                self.planes.append(("k", c, layer, base, extra))
            if fine:
                self.planes.append(("m", 0, layer, 1, 0))
            if depth < 2:
                for c in range(3):
                    self.planes.append(("p", c, layer, 0, 2))
                self.planes.append(("d", 0, layer, 0, 2))
        self.index = {plane[:3]: i for i, plane in enumerate(self.planes)}

    def depth(self, layer):
        return self.layers - 1 - layer if self.fine else layer

    def x_tiles(self):
        return -(-len(self.planes) // SLOTS) * (self.row_tiles + 1)


def row_table(blocks):
    base, extra, at = {}, {}, 0
    for count in (2, 1):
        for b, block in enumerate(blocks):
            for p, plane in enumerate(block.planes):
                if plane[3] == count:
                    for t in range(block.col_tiles):
                        base[b, p, t] = slice(at, at + count)
                        at += count
    start, ends = at, []
    for b, block in enumerate(blocks):
        at = start
        for count in (2, 1):
            for p, plane in enumerate(block.planes):
                if plane[4] == count:
                    for t in range(block.col_tiles):
                        extra[b, p, t] = slice(at, at + count)
                        at += count
        ends.append(at)
    return base, extra, -(-max(ends) // SUB) * SUB


def lanes_of(t):
    return slice(LANE * t, LANE * t + LANE)


def rows_of(t):
    return slice(SUB * t, SUB * t + SUB)


def own(refs, plane, rows, lanes):
    kind, c, layer = plane[:3]
    if kind in ("m", "d"):
        return refs[kind][layer, rows, lanes]
    return refs[kind][c, layer, rows, lanes]


def is_even(axis):
    return lax.rem(lax.axis_index(axis), 2) == 0


def iota(shape, dim):
    return lax.broadcasted_iota(jnp.int32, shape, dim)


def named(refs):
    fine = dict(zip("ukmpd", refs[:5]))
    coarse = dict(zip("ukpd", refs[5:9]))
    return (fine, coarse), refs[9:]


def rows_kernel(blocks, *refs):
    held, loaded = refs[:9], refs[9:18]
    first, second, face_first, face_second, done = refs[18:]
    copies = [
        pltpu.make_async_copy(source, target, done.at[i])
        for i, (source, target) in enumerate(zip(held, loaded))
    ]
    for copy in copies:
        copy.start()
    for copy in copies:
        copy.wait()
    sources, _ = named(loaded)
    base, extra, _ = row_table(blocks)
    even = is_even("gy")
    is_low = lax.axis_index("gz") == 0

    def move(b, block, plane, at, t, near, far):
        high = own(sources[b], plane, slice(block.rows - far, block.rows - near), lanes_of(t))
        low = own(sources[b], plane, slice(near, far), lanes_of(t))
        first[at, :] = lax.select(even, high, low)
        second[at, :] = lax.select(even, low, high)

    for b, block in enumerate(blocks):
        for p, plane in enumerate(block.planes):
            for t in range(block.col_tiles):
                if plane[3]:
                    move(b, block, plane, base[b, p, t], t, 0, plane[3])
    for b, block in enumerate(blocks):

        @pl.when(is_low != block.fine)
        def _():
            for p, plane in enumerate(block.planes):
                for t in range(block.col_tiles):
                    if plane[4]:
                        move(b, block, plane, extra[b, p, t], t, plane[3], plane[3] + plane[4])

    even = is_even("gz")
    at = 0
    for b, block in enumerate(blocks):
        for c in range(3):
            for rt in range(block.row_tiles):
                for ct in range(block.col_tiles):
                    low = sources[b]["u"][c, 0, rows_of(rt), lanes_of(ct)]
                    high = sources[b]["u"][c, block.layers - 1, rows_of(rt), lanes_of(ct)]
                    face_first[at] = lax.select(even, high, low)
                    face_second[at] = lax.select(even, low, high)
                    at += 1


def columns_kernel(blocks, both, *refs):
    sources, rest = named(refs)
    got_first, got_second = rest[:2]
    halos = rest[2:4]
    outs = rest[4:]
    base, extra, _ = row_table(blocks)
    even = is_even("gy")
    is_low = lax.axis_index("gz") == 0

    def place(b, p, at, t, near, far):
        one, two = got_first[at, :], got_second[at, :]
        halos[b][p, near:far, lanes_of(t)] = lax.select(even, one, two)
        halos[b][p, SUB - far : SUB - near, lanes_of(t)] = lax.select(even, two, one)

    for b, block in enumerate(blocks):
        for p, plane in enumerate(block.planes):
            halos[b][p] = jnp.zeros((SUB, block.cols), jnp.float32)
            for t in range(block.col_tiles):
                if plane[3]:
                    place(b, p, base[b, p, t], t, 0, plane[3])
    for b, block in enumerate(blocks):

        @pl.when(is_low != block.fine)
        def _():
            for p, plane in enumerate(block.planes):
                for t in range(block.col_tiles):
                    if plane[4]:
                        place(b, p, extra[b, p, t], t, plane[3], plane[3] + plane[4])

    even = is_even("gx")
    lane = iota((SUB, LANE), 1)
    slot = lax.shift_right_logical(lane, jnp.full((SUB, LANE), 2, jnp.int32))
    move = lax.select(even, jnp.int32(COLS), jnp.int32(0))
    back = COLS - move
    at = 0
    for b, block in enumerate(blocks):
        for group in range(0, len(block.planes), SLOTS):
            for rt in range(block.row_tiles + 1):
                made = [jnp.zeros((SUB, LANE), jnp.float32) for _ in outs]
                for s, plane in enumerate(block.planes[group : group + SLOTS]):
                    if rt < block.row_tiles:
                        left = own(sources[b], plane, rows_of(rt), lanes_of(0))
                        right = own(sources[b], plane, rows_of(rt), lanes_of(block.col_tiles - 1))
                    elif plane[3] + plane[4]:
                        left = halos[b][group + s, :, lanes_of(0)]
                        right = halos[b][group + s, :, lanes_of(block.col_tiles - 1)]
                    else:
                        continue
                    for o in range(len(outs)):
                        face = lax.select(even, right, left) if o == 0 else lax.select(even, left, right)
                        by = lax.rem(COLS * s + (move if o == 0 else back), LANE)
                        made[o] = jnp.where(slot == s, pltpu.roll(face, by, 1), made[o])
                for o, out in enumerate(outs):
                    out[at] = made[o]
                at += 1


def put(buffer, at, value):
    rows, cols = value.shape
    for rt in range(rows // SUB):
        for ct in range(cols // LANE):
            buffer[at] = value[rows_of(rt), lanes_of(ct)]
            at += 1
    return at


def take(read, at, rows, cols):
    tiles = [
        jnp.concatenate(
            [read(at + rt * (cols // LANE) + ct) for ct in range(cols // LANE)], axis=1
        )
        for rt in range(rows // SUB)
    ]
    return jnp.concatenate(tiles, axis=0), at + (rows // SUB) * (cols // LANE)


def slope(value, dim):
    size = value.shape[dim]
    return pltpu.roll(value, size - 1, dim) - pltpu.roll(value, 1, dim)


def signed(index, inner, total):
    return jnp.where(index < (inner + total) // 2, index, index - total)


def split_dot(value, matrix):
    high = value.astype(jnp.bfloat16)
    rest = value - high.astype(jnp.float32)
    middle = rest.astype(jnp.bfloat16)
    low = (rest - middle.astype(jnp.float32)).astype(jnp.bfloat16)
    parts = jnp.concatenate([high, middle, low], axis=0)
    out = jnp.dot(parts, matrix.astype(jnp.bfloat16), preferred_element_type=jnp.float32)
    rows = value.shape[0]
    return out[:rows] + (out[rows : 2 * rows] + out[2 * rows :])


def restrict(planes, spare, fine, coarse):
    rows, cols = fine.rows, fine.cols
    row = iota((SUB, fine.wide[1]), 0)
    stacked = []
    for i, plane in enumerate(planes):
        inner = []
        for t in range(fine.col_tiles + 1):
            at = (i * (fine.col_tiles + 1) + t) * rows
            spare[at : at + rows, :] = plane[:rows, lanes_of(t)]
            even = spare[pl.ds(at, coarse.rows, 2), :]
            inner.append(even + spare[pl.ds(at + 1, coarse.rows, 2), :])
        inner = jnp.concatenate(inner, axis=1)
        pair = plane[rows:]
        pair = pair + pltpu.roll(pair, SUB - 1, 0)
        outer = jnp.where(row == 0, pair, 0.0)
        for to, by in ((1, SUB - 1), (6, 2), (7, 1)):
            outer = jnp.where(row == to, pltpu.roll(pair, by, 0), outer)
        stacked += [inner, outer]
    stacked = 0.25 * jnp.concatenate(stacked, axis=0)
    inner = jnp.right_shift(iota((cols, coarse.cols), 0), 1) == iota((cols, coarse.cols), 1)
    f = signed(iota((LANE, LANE), 0), 0, LANE)
    outer = jnp.right_shift(f, 1) == signed(iota((LANE, LANE), 1), 0, LANE)
    ones = lambda where: jnp.where(where, 1.0, 0.0)
    out = jnp.concatenate(
        [split_dot(stacked[:, :cols], ones(inner)), split_dot(stacked[:, cols:], ones(outer))],
        axis=1,
    )
    height = coarse.wide[0]
    return [out[i * height : i * height + height] for i in range(len(planes))]


def prolong(planes, spare, fine, coarse):
    shape = (coarse.wide[1], fine.wide[1])
    c = signed(iota(shape, 0), coarse.cols, shape[0])
    f = signed(iota(shape, 1), fine.cols, shape[1])
    half = jnp.right_shift(f, 1)
    other = half - 1 + 2 * jnp.bitwise_and(f, 1)
    by_x = jnp.where(half == c, 0.75, jnp.where(other == c, 0.25, 0.0))
    height, rows = coarse.wide[0], coarse.rows
    stacked = split_dot(jnp.concatenate(planes, axis=0), by_x)
    row = iota((SUB, shape[1]), 0)
    out = []
    for i in range(len(planes)):
        value = stacked[i * height : i * height + height]
        even = 0.75 * value + 0.25 * pltpu.roll(value, 1, 0)
        odd = 0.75 * value + 0.25 * pltpu.roll(value, height - 1, 0)
        inner = []
        for t in range(fine.col_tiles + 1):
            at = (i * (fine.col_tiles + 1) + t) * 2 * rows
            spare[pl.ds(at, rows, 2), :] = even[:rows, lanes_of(t)]
            spare[pl.ds(at + 1, rows, 2), :] = odd[:rows, lanes_of(t)]
            inner.append(spare[at : at + 2 * rows, :])
        inner = jnp.concatenate(inner, axis=1)
        even, odd = even[rows:], odd[rows:]
        outer = jnp.where(row == 0, even, odd)
        for to, by, kind in (
            (1, 1, odd), (2, 1, even), (3, 2, odd), (4, 6, even), (5, 7, odd), (6, 7, even)
        ):
            outer = jnp.where(row == to, pltpu.roll(kind, by, 0), outer)
        out.append(jnp.concatenate([inner, outer], axis=0))
    return out


def clamp(plane, coarse):
    for axis, dim, inner in (("gy", 0, coarse.rows), ("gx", 1, coarse.cols)):
        spot, count = lax.axis_index(axis), lax.axis_size(axis)
        index = signed(iota(plane.shape, dim), inner, plane.shape[dim])
        low = lax.slice_in_dim(plane, 0, 1, axis=dim)
        high = lax.slice_in_dim(plane, inner - 1, inner, axis=dim)
        least = lax.select(spot == 0, jnp.int32(0), jnp.int32(-plane.shape[dim]))
        most = lax.select(spot == count - 1, jnp.int32(inner - 1), jnp.int32(plane.shape[dim]))
        plane = jnp.where(index < least, low, jnp.where(index > most, high, plane))
    return plane


def wide_tiles(count, coarse):
    inner = coarse.row_tiles * coarse.col_tiles
    return count * inner + -(-count // 2) * coarse.col_tiles + coarse.row_tiles + 1


def put_wide(buffer, at, planes, coarse):
    rows, cols = coarse.rows, coarse.cols
    for value in planes:
        at = put(buffer, at, value[:rows, :cols])
    for ct in range(coarse.col_tiles):
        for i, value in enumerate(planes):
            to = 4 * (i % 2)
            buffer[at + i // 2, to : to + 2] = value[rows : rows + 2, lanes_of(ct)]
            buffer[at + i // 2, to + 2 : to + 4] = value[rows + SUB - 2 :, lanes_of(ct)]
        at += -(-len(planes) // 2)
    slot = jnp.right_shift(iota((SUB, LANE), 1), 2)
    for rt in range(coarse.row_tiles + 1):
        tile = jnp.zeros((SUB, LANE), jnp.float32)
        for i, value in enumerate(planes):
            tile = jnp.where(slot == i, pltpu.roll(value[rows_of(rt), cols:], 2 + 4 * i, 1), tile)
        buffer[at] = tile
        at += 1
    return at


def take_wide(buffer, at, count, coarse):
    row, lane = iota((SUB, LANE), 0), iota((SUB, LANE), 1)
    read = lambda spot: buffer[spot]
    inner = []
    for _ in range(count):
        value, at = take(read, at, coarse.rows, coarse.cols)
        inner.append(value)
    ends = [[] for _ in range(count)]
    for ct in range(coarse.col_tiles):
        for i in range(count):
            tile = buffer[at + i // 2]
            start = 4 * (i % 2)
            ahead = pltpu.roll(tile, (SUB - start) % SUB, 0)
            behind = pltpu.roll(tile, 4 - start, 0)
            ends[i].append(jnp.where(row < 2, ahead, jnp.where(row >= SUB - 2, behind, 0.0)))
        at += -(-count // 2)
    sides = [[] for _ in range(count)]
    for rt in range(coarse.row_tiles + 1):
        for i in range(count):
            tile = pltpu.roll(buffer[at], LANE - 2 - 4 * i, 1)
            sides[i].append(jnp.where((lane < 2) | (lane >= LANE - 2), tile, 0.0))
        at += 1
    planes = []
    for i in range(count):
        left = jnp.concatenate([inner[i], jnp.concatenate(ends[i], axis=1)], axis=0)
        planes.append(jnp.concatenate([left, jnp.concatenate(sides[i], axis=0)], axis=1))
    return planes, at


def interface_tiles(fine, coarse):
    top = wide_tiles(3, coarse) + 3 * coarse.row_tiles * coarse.col_tiles
    return max(top + 3 * fine.row_tiles * fine.col_tiles, wide_tiles(9, coarse))


def face_tiles(blocks):
    return sum(3 * b.row_tiles * b.col_tiles for b in blocks)


def edge_tiles(blocks):
    return sum(b.row_tiles + b.col_tiles for b in blocks)


def neighbours(first, second):
    even = is_even("gz")
    return (
        lambda at: lax.select(even, second[at], first[at]),
        lambda at: lax.select(even, first[at], second[at]),
    )


def widen(blocks, sources, halos, got, wides):
    even = is_even("gx")
    lane = iota((SUB, LANE), 1)
    shift = lax.select(even, jnp.int32(0), jnp.int32(COLS))
    masks = [
        jnp.bitwise_and(lane + shift, LANE - 1) < COLS,
        jnp.bitwise_and(lane + COLS - shift, LANE - 1) < COLS,
    ]
    start = 0
    for b, block in enumerate(blocks):
        rows, cols = block.rows, block.cols
        for p, plane in enumerate(block.planes):
            wide = wides[b]
            wide[p, 0:rows, 0:cols] = own(sources[b], plane, slice(0, rows), slice(0, cols))
            wide[p, rows:, 0:cols] = halos[b][p]
            s = p % SLOTS
            at = start + (p // SLOTS) * (block.row_tiles + 1)
            for rt in range(block.row_tiles + 1):
                tile = jnp.zeros((SUB, LANE), jnp.float32)
                for o, buffer in enumerate(got):
                    by = shift if o == 0 else COLS - shift
                    moved = pltpu.roll(buffer[at + rt], lax.rem(2 * LANE - COLS * s - by, LANE), 1)
                    tile = tile + jnp.where(masks[o], moved, 0.0)
                wide[p, rows_of(rt), cols:] = tile
        start += block.x_tiles()


def step_kernel(blocks, x_count, *refs):
    sources, rest = named(refs)
    halos, face_first, face_second, rest = rest[:2], rest[2], rest[3], rest[2:]
    got = rest[2 : 2 + x_count]
    steps_out = rest[2 + x_count : 4 + x_count]
    first, second, coefs, coefs_coarse, keep = rest[4 + x_count : 9 + x_count]
    wides = rest[9 + x_count : 11 + x_count]
    stresses = rest[11 + x_count : 13 + x_count]
    starts = rest[13 + x_count : 15 + x_count]
    spare = rest[15 + x_count]
    all_coefs = (coefs, coefs_coarse)
    spot_z, count_z = lax.axis_index("gz"), lax.axis_size("gz")
    even = is_even("gz")
    widen(blocks, sources, halos, got, wides)
    before, after = neighbours(face_first, face_second)

    start = 0
    for b, block in enumerate(blocks):
        beyond = [[], []]
        for c in range(3):
            for side, read in enumerate((before, after)):
                plane, _ = take(read, start, block.rows, block.cols)
                plane = jnp.concatenate([plane, jnp.zeros((SUB, block.cols), jnp.float32)], axis=0)
                plane = jnp.concatenate([plane, jnp.zeros((block.wide[0], LANE), jnp.float32)], axis=1)
                beyond[side].append(plane)
            start += block.row_tiles * block.col_tiles
        wide, stress = wides[b], stresses[b]
        layers, rows, cols, inverse = block.layers, block.rows, block.cols, block.inverse_step
        half = count_z * layers // 2

        def field(kind, c, layer):
            return wide[block.index[kind, c, layer]]

        def stretched(layer, inner=False):
            if not block.fine:
                return None
            value = field("m", 0, layer)
            if inner:
                value = value[:rows, :cols]
            return lax.select(spot_z * layers + layer < half, value, jnp.ones_like(value))

        def along_z(below, above, stretch):
            if below is None:
                value = above
            elif above is None:
                value = -below
            else:
                value = above - below
            value = value * inverse
            return value if stretch is None else value * stretch

        for layer in range(layers):
            k = [functools.partial(field, "k", c, layer) for c in range(9)]
            u = [field("u", c, layer) for c in range(3)]
            stretch = stretched(layer)
            dz = [
                along_z(
                    field("u", c, layer - 1) if layer else beyond[0][c],
                    field("u", c, layer + 1) if layer < layers - 1 else beyond[1][c],
                    stretch,
                )
                for c in range(3)
            ]
            nx = slope(u[0], 1) * inverse
            ny = slope(u[1], 0) * inverse
            nz = dz[2]
            stress[XX, layer] = k[0]() * nx + k[6]() * ny + k[7]() * nz
            stress[YY, layer] = k[6]() * nx + k[1]() * ny + k[8]() * nz
            stress[ZZ, layer] = k[7]() * nx + k[8]() * ny + k[2]() * nz
            stress[YZ, layer] = k[3]() * (dz[1] + slope(u[2], 0) * inverse)
            stress[XZ, layer] = k[4]() * (dz[0] + slope(u[2], 1) * inverse)
            stress[XY, layer] = k[5]() * ((slope(u[0], 0) + slope(u[1], 1)) * inverse)

        for side, layer in enumerate((0, layers - 1)):
            stretch = stretched(layer)
            for i, c in enumerate((4, 3, 2, 7, 8)):
                value = field("k", c, layer) * inverse
                all_coefs[b][side, i] = value if stretch is None else value * stretch

        table = ((XX, XY, XZ), (XY, YY, YZ), (XZ, YZ, ZZ))
        for layer in range(layers):
            depth = block.depth(layer)
            stretch = stretched(layer, depth >= 2)
            for c in range(3):
                part = table[c]
                height, width = (slice(0, None),) * 2 if depth < 2 else (slice(0, rows), slice(0, cols))
                dx = slope(stress[part[0], layer, height, :], 1)[:, width] * inverse
                dy = slope(stress[part[1], layer, :, width], 0)[height] * inverse
                dz = along_z(
                    stress[part[2], layer - 1, height, width] if layer else None,
                    stress[part[2], layer + 1, height, width] if layer < layers - 1 else None,
                    stretch,
                )
                if depth < 2:
                    now, prev = field("u", c, layer), field("p", c, layer)
                    density = field("d", 0, layer)
                    density = jnp.where(density > 0, density, 1.0)
                else:
                    now = sources[b]["u"][c, layer]
                    prev = sources[b]["p"][c, layer]
                    density = sources[b]["d"][layer]
                value = (2.0 * now - prev) + ALPHA * (dx + dy + dz) / density
                steps_out[b][c, layer] = value[:rows, :cols]
                if depth == 0:
                    starts[b][c] = value
                elif depth == 1 and block.fine:
                    keep[c] = value
                elif depth == 1:
                    starts[b][3 + c] = value

    fine, coarse = blocks
    for i, c in enumerate((4, 3, 2)):
        keep[3 + i] = wides[0][fine.index["k", c, fine.layers - 1]]

    at = 0
    lane = iota((SUB, LANE), 1)

    def send(tile_low, tile_high):
        nonlocal at
        first[at] = lax.select(even, tile_high, tile_low)
        second[at] = lax.select(even, tile_low, tile_high)
        at += 1

    for b, block in enumerate(blocks):
        last = block.layers - 1
        rows, cols = block.rows, block.cols
        for rt in range(block.row_tiles):
            for ct in range(block.col_tiles):
                spot = (rows_of(rt), lanes_of(ct))
                for kind in (XZ, YZ, ZZ):
                    send(stresses[b][(kind, 0) + spot], stresses[b][(kind, last) + spot])
        for ct in range(block.col_tiles):
            for c in range(3):
                low = block.index["u", c, 0]
                high = block.index["u", c, last]
                for edge, to in ((rows, c), (rows + SUB - 1, 4 + c)):
                    one = wides[b][low, edge : edge + 1, lanes_of(ct)]
                    two = wides[b][high, edge : edge + 1, lanes_of(ct)]
                    first[at, to : to + 1] = lax.select(even, two, one)
                    second[at, to : to + 1] = lax.select(even, one, two)
            at += 1
        for rt in range(block.row_tiles):
            pair = [jnp.zeros((SUB, LANE), jnp.float32)] * 2
            for c in range(3):
                for side, layer in enumerate((0, last)):
                    halo = wides[b][block.index["u", c, layer], rows_of(rt), cols:]
                    pair[side] = jnp.where(
                        jnp.right_shift(lane, 1) == c, pltpu.roll(halo, 1 + 2 * c, 1), pair[side]
                    )
            send(*pair)

    @pl.when(spot_z == count_z - 1)
    def _():
        planes = [starts[0][c] for c in range(3)] + [keep[c] for c in range(3)]
        down = restrict(planes, spare, fine, coarse)
        at = put_wide(second, 0, down[:3], coarse)
        for plane in down[3:]:
            at = put(second, at, plane[: coarse.rows, : coarse.cols])
        for c in range(3):
            at = put(second, at, keep[3 + c][: fine.rows, : fine.cols])

    @pl.when(spot_z == 0)
    def _():
        planes = [[], [], []]
        for i, c in enumerate((4, 3, 2)):
            k = wides[1][coarse.index["k", c, 0]]
            start, below = starts[1][i], starts[1][3 + i]
            planes[0].append(k * (below - start) * 0.25)
            planes[1].append(k * (below - 0.5 * start) * 0.25)
            planes[2].append(k * 0.125)
        put_wide(second, 0, sum(planes, []), coarse)


def last_kernel(blocks, *refs):
    (step_f, step_c, coef_f, coef_c, got_first, got_second, sent, keep) = refs[:8]
    metric, density_f, density_c = refs[8:11]
    outs, spare = refs[11:13], refs[13]
    fine, coarse = blocks
    spot_z, count_z = lax.axis_index("gz"), lax.axis_size("gz")
    lane, row = iota((SUB, LANE), 1), iota((SUB, LANE), 0)

    def inside(read, there):
        def masked(at):
            value = read(at)
            return lax.select(there, value, jnp.zeros_like(value))

        return masked

    before, after = neighbours(got_first, got_second)
    readers = inside(before, spot_z > 0), inside(after, spot_z < count_z - 1)

    start = 0
    for b, block in enumerate(blocks):
        rows, cols, layers, inverse = block.rows, block.cols, block.layers, block.inverse_step
        half = count_z * layers // 2
        step = (step_f, step_c)[b]
        density = (density_f, density_c)[b]
        coef = (coef_f, coef_c)[b]
        out = outs[b]
        extra = {}

        def add(c, layer, value):
            extra[c, layer] = extra[c, layer] + value if (c, layer) in extra else value

        def stretched(layer, value):
            value = value * inverse
            if not block.fine:
                return value
            factor = metric[layer]
            factor = lax.select(
                spot_z * layers + layer < half, factor, jnp.ones_like(factor)
            )
            return value * factor

        for side, layer in enumerate((0, layers - 1)):
            read = readers[side]
            sign = -1.0 if side == 0 else 1.0
            tiles = block.row_tiles * block.col_tiles
            beyond = []
            for c in range(3):
                edges = []
                for ct in range(block.col_tiles):
                    tile = read(start + 3 * tiles + ct)
                    ahead = pltpu.roll(tile, (SUB - c) % SUB, 0)
                    behind = pltpu.roll(tile, 3 - c, 0)
                    edges.append(
                        jnp.where(row == 0, ahead, jnp.where(row == SUB - 1, behind, 0.0))
                    )
                sides = []
                for rt in range(block.row_tiles):
                    tile = read(start + 3 * tiles + block.col_tiles + rt)
                    tile = pltpu.roll(tile, LANE - 1 - 2 * c, 1)
                    sides.append(jnp.where((lane == 0) | (lane == LANE - 1), tile, 0.0))
                beyond.append(
                    (
                        sign * jnp.concatenate(edges, axis=1),
                        sign * jnp.concatenate(sides, axis=0),
                    )
                )

            def over_x(k, value):
                halo = coef[side, k, :rows, cols:] * value
                left = jnp.zeros((rows, cols), jnp.float32)
                return slope(jnp.concatenate([left, halo], axis=1), 1)[:, :cols] * inverse

            def over_y(k, value):
                halo = coef[side, k, rows:, :cols] * value
                left = jnp.zeros((rows, cols), jnp.float32)
                return slope(jnp.concatenate([left, halo], axis=0), 0)[:rows] * inverse

            add(0, layer, over_x(3, beyond[2][1]))
            add(1, layer, over_y(4, beyond[2][0]))
            add(2, layer, over_x(0, beyond[0][1]) + over_y(1, beyond[1][0]))
            for c in range(3):
                there = jnp.concatenate(
                    [
                        jnp.concatenate(
                            [
                                read(start + 3 * (rt * block.col_tiles + ct) + c)
                                for ct in range(block.col_tiles)
                            ],
                            axis=1,
                        )
                        for rt in range(block.row_tiles)
                    ],
                    axis=0,
                )
                add(c, layer, stretched(layer, sign * there))
        for layer in range(layers):
            for c in range(3):
                value = step[c, layer]
                if (c, layer) in extra:
                    value = value + ALPHA * extra[c, layer] / density[layer]
                out[c, layer] = value
        start += 3 * block.row_tiles * block.col_tiles + block.row_tiles + block.col_tiles

    @pl.when(spot_z == count_z - 1)
    def _():
        part, _ = take_wide(got_second, 0, 9, coarse)
        above = [keep[c] for c in range(3)]
        k = [jnp.where(keep[3 + c] > 0, keep[3 + c], 1.0) for c in range(3)]
        raised = prolong([clamp(part[c], coarse) for c in range(3)], spare, fine, coarse)
        down = restrict([above[c] + raised[c] / k[c] for c in range(3)], spare, fine, coarse)
        tractions = [clamp(part[3 + c] - part[6 + c] * down[c], coarse) for c in range(3)]
        raised = prolong(tractions, spare, fine, coarse)
        for c in range(3):
            value = above[c] + raised[c] / k[c]
            outs[0][c, fine.layers - 1] = value[: fine.rows, : fine.cols]

    @pl.when(spot_z == 0)
    def _():
        read = lambda spot: got_second[spot]
        down, at = take_wide(got_second, 0, 3, coarse)
        part, _ = take_wide(sent, 0, 9, coarse)
        tractions = [clamp(part[3 + c] - part[6 + c] * down[c], coarse) for c in range(3)]
        raised = prolong(tractions, spare, fine, coarse)
        above = []
        for c in range(3):
            value, at = take(read, at, coarse.rows, coarse.cols)
            above.append(value)
        shares = []
        for c in range(3):
            k, at = take(read, at, fine.rows, fine.cols)
            share = raised[c][: fine.rows, : fine.cols] / k
            share = jnp.concatenate(
                [share, jnp.zeros((SUB, fine.cols), jnp.float32)], axis=0
            )
            shares.append(
                jnp.concatenate(
                    [share, jnp.zeros((fine.wide[0], LANE), jnp.float32)], axis=1
                )
            )
        down = restrict(shares, spare, fine, coarse)
        for c in range(3):
            total = above[c] + down[c][: coarse.rows, : coarse.cols]
            outs[1][c, 0] = 0.5 * (step_c[c, 0] + total)


def pair_tables(count):
    even = [(i, i + 1) for i in range(0, count - 1, 2)]
    odd = [(i, i + 1) for i in range(1, count - 1, 2)]
    both = lambda some: some + [(b, a) for a, b in some]
    return both(even), both(odd)


def f32(*shape):
    return jax.ShapeDtypeStruct(shape, jnp.float32)


def kernel(body, out_shape, count, scratch=(), held=False):
    space = pl.BlockSpec(memory_space=pltpu.VMEM)
    outside = pl.BlockSpec(memory_space=pltpu.HBM) if held else space
    scratches = [pltpu.VMEM(shape, jnp.float32) for shape in scratch]
    if held:
        scratches = [pltpu.SemaphoreType.DMA((count,))]
    return pl.pallas_call(
        body,
        out_shape=out_shape,
        in_specs=[outside] * count,
        out_specs=[space] * len(out_shape),
        scratch_shapes=scratches,
        compiler_params=pltpu.CompilerParams(vmem_limit_bytes=VMEM_BYTES),
    )


def per_device(
    fine_now,
    fine_prev,
    stiffness,
    metric,
    density,
    coarse_now,
    coarse_prev,
    coarse_stiffness,
    coarse_density,
):
    blocks = fine, coarse = (
        Block(fine_now.shape[1:], True),
        Block(coarse_now.shape[1:], False),
    )
    arrays = [
        fine_now, stiffness, metric, fine_prev, density,
        coarse_now, coarse_stiffness, coarse_prev, coarse_density,
    ]
    count_z = lax.axis_size("gz")
    assert count_z % 2 == 0

    _, _, row_count = row_table(blocks)
    face_shape = f32(face_tiles(blocks), SUB, LANE)
    *arrays, first, second, face_first, face_second = kernel(
        functools.partial(rows_kernel, blocks),
        [f32(*array.shape) for array in arrays]
        + [f32(row_count, LANE)] * 2
        + [face_shape] * 2,
        len(arrays),
        held=True,
    )(*[pltpu.with_memory_space_constraint(array, pltpu.HBM) for array in arrays])
    by_row = [
        lax.ppermute(buffer, "gy", pairs) if pairs else jnp.zeros_like(buffer)
        for buffer, pairs in zip((first, second), pair_tables(lax.axis_size("gy")))
    ]

    even_pairs, odd_pairs = pair_tables(count_z)

    def swap_z(first, second):
        if odd_pairs:
            got = lax.ppermute(second, "gz", odd_pairs)
        else:
            got = jnp.zeros_like(second)
        return lax.ppermute(first, "gz", even_pairs), got

    faces = swap_z(face_first, face_second)

    tables = [pairs for pairs in pair_tables(lax.axis_size("gx")) if pairs]
    tiles = sum(block.x_tiles() for block in blocks)
    halo_shapes = [f32(len(block.planes), SUB, block.cols) for block in blocks]
    made = kernel(
        functools.partial(columns_kernel, blocks, len(tables)),
        halo_shapes + [f32(tiles, SUB, LANE)] * len(tables),
        11,
    )(*arrays, *by_row)
    halos = made[:2]
    by_column = [
        lax.ppermute(buffer, "gx", pairs) for buffer, pairs in zip(made[2:], tables)
    ]

    count = max(face_tiles(blocks) + edge_tiles(blocks), interface_tiles(*blocks))
    z_shape = f32(count, SUB, LANE)
    step_f, step_c, first, second, coef_f, coef_c, keep = kernel(
        functools.partial(step_kernel, blocks, len(tables)),
        [f32(*fine_now.shape), f32(*coarse_now.shape), z_shape, z_shape]
        + [f32(2, 5, *block.wide) for block in blocks]
        + [f32(6, *fine.wide)],
        13 + len(tables),
        [(len(block.planes), *block.wide) for block in blocks]
        + [(6, block.layers, *block.wide) for block in blocks]
        + [(3, *fine.wide), (6, *coarse.wide)]
        + [(6 * (fine.col_tiles + 1) * fine.rows, LANE)],
    )(*arrays, *halos, *faces, *by_column)
    with jax.named_scope("z_second"):
        got_second = lax.ppermute(
            second, "gz", odd_pairs + [(0, count_z - 1), (count_z - 1, 0)]
        )
    with jax.named_scope("z_first"):
        got_first = lax.ppermute(first, "gz", even_pairs)

    metric, density, density_c = arrays[2], arrays[4], arrays[8]
    return tuple(
        kernel(
            functools.partial(last_kernel, blocks),
            [f32(*fine_now.shape), f32(*coarse_now.shape)],
            11,
            [(3 * (fine.col_tiles + 1) * fine.rows, LANE)],
        )(
            step_f, step_c, coef_f, coef_c, got_first, got_second, second, keep,
            metric, density, density_c,
        )
    )


def solution(mesh):
    block = P(None, "gz", "gy", "gx")
    field = P("gz", "gy", "gx")
    return jax.shard_map(
        per_device,
        mesh=mesh,
        in_specs=(block, block, block, field, field, block, block, block, field),
        out_specs=(block, block),
        check_vma=False,
    )
```
